256 devices in a mesh: gx: 16 (over z, core), gy: 16 (over x, y).
Axes of the slice: x: 4, y: 4, z: 8, core: 2. Of those that a mesh axis runs over, the one named last changes fastest.
Arguments:
- density: float32 [256, 256, 128], P('gx', 'gy'), may hold values from 0.05 to 40, as said below
Outputs:
- potential: float32 [256, 256, 128], P('gx', 'gy')
The draws below stay inside these ranges and needn't reach their ends.
Inputs may be any that keep to these rules, and one draw needn't show every extreme that they name: `density`: densities are positive.
All inputs are finite; a program needn't handle non-finite values.
Results may differ from the reference program's by a relative error of at most 0.00014.
Values sent between devices are 32-bit elements; how exact they have to be, the bound alone decides.
A program may use at most 64 MiB of HBM per device.

```python
import jax
import jax.numpy as jnp

LEVELS = 4
NEWTON = 3
COARSE_SWEEPS = 2
NX = 256
NY = 256
NZ = 128


def draw_density(key, part):
    noise_key = jax.random.fold_in(jax.random.fold_in(key, 17), 0)
    noise_draw = jnp.clip(jax.random.normal(noise_key, (NX, NY, NZ), jnp.float32), -4.0, 4.0)
    coord_x = jnp.arange(NX, dtype=jnp.float32) / NX
    coord_y = jnp.arange(NY, dtype=jnp.float32) / NY
    tilt_factor = (1.0 + coord_x)[:, None, None] * (1.0 + coord_y)[None, :, None]
    density_field = jnp.exp(0.3 * noise_draw) * tilt_factor
    return density_field.astype(jnp.float32)


def setup_inputs(seed: int = 0) -> dict:
    key_of = jax.random.split(jax.random.key(seed), 2)
    return {
        "density": draw_density(jax.random.fold_in(key_of[1], 71), 0),
    }


COUPLING = 0.1
FLOOR = 3.0


def shifted(padded, off_x, off_y, off_z):
    size_x = padded.shape[0] - 2
    size_y = padded.shape[1] - 2
    size_z = padded.shape[2] - 2
    return padded[1 + off_x:1 + off_x + size_x, 1 + off_y:1 + off_y + size_y, 1 + off_z:1 + off_z + size_z]


def hessian(padded, spacing_inv):
    center = shifted(padded, 0, 0, 0)
    pure_x = (shifted(padded, 1, 0, 0) + shifted(padded, -1, 0, 0) - 2.0 * center) * spacing_inv
    pure_y = (shifted(padded, 0, 1, 0) + shifted(padded, 0, -1, 0) - 2.0 * center) * spacing_inv
    pure_z = (shifted(padded, 0, 0, 1) + shifted(padded, 0, 0, -1) - 2.0 * center) * spacing_inv
    quarter = 0.25 * spacing_inv
    mixed_xy = (shifted(padded, 1, 1, 0) - shifted(padded, 1, -1, 0) - shifted(padded, -1, 1, 0) + shifted(padded, -1, -1, 0)) * quarter
    mixed_xz = (shifted(padded, 1, 0, 1) - shifted(padded, 1, 0, -1) - shifted(padded, -1, 0, 1) + shifted(padded, -1, 0, -1)) * quarter
    mixed_yz = (shifted(padded, 0, 1, 1) - shifted(padded, 0, 1, -1) - shifted(padded, 0, -1, 1) + shifted(padded, 0, -1, -1)) * quarter
    return pure_x, pure_y, pure_z, mixed_xy, mixed_xz, mixed_yz


def nonlinear(padded, source):
    pure_x, pure_y, pure_z, mixed_xy, mixed_xz, mixed_yz = hessian(padded, 1.0)
    cubic = 2.0 * (pure_x * pure_y + pure_x * pure_z + pure_y * pure_z - mixed_xy * mixed_xy - mixed_xz * mixed_xz - mixed_yz * mixed_yz)
    return pure_x + pure_y + pure_z + COUPLING * cubic - source


def coefficients(padded, spacing_inv):
    pure_x, pure_y, pure_z, mixed_xy, mixed_xz, mixed_yz = hessian(padded, spacing_inv)
    stiff_x = 1.0 + 2.0 * COUPLING * (pure_y + pure_z)
    stiff_y = 1.0 + 2.0 * COUPLING * (pure_x + pure_z)
    stiff_z = 1.0 + 2.0 * COUPLING * (pure_x + pure_y)
    diagonal = jnp.maximum(2.0 * (stiff_x + stiff_y + stiff_z), FLOOR)
    relax = 1.0 / (spacing_inv * diagonal)
    return jnp.stack([stiff_x, stiff_y, stiff_z, -4.0 * COUPLING * mixed_xy, -4.0 * COUPLING * mixed_xz, -4.0 * COUPLING * mixed_yz, relax])


def jacobian(padded, weights, spacing_inv):
    parts = hessian(padded, spacing_inv)
    result = weights[0] * parts[0]
    for index in range(1, 6):
        result = result + weights[index] * parts[index]
    return result


def restrict(field):
    size_x, size_y, size_z = field.shape
    blocks = field.reshape(size_x // 2, 2, size_y // 2, 2, size_z // 2, 2)
    return jnp.sum(blocks, axis=(1, 3, 5)) * 0.125


def prolong(field):
    size_x, size_y, size_z = field.shape
    spread = jnp.broadcast_to(field[:, None, :, None, :, None], (size_x, 2, size_y, 2, size_z, 2))
    return spread.reshape(2 * size_x, 2 * size_y, 2 * size_z)


def wrap_all(field):
    return jnp.pad(field, 1, mode="wrap")


def checker(shape, first_x, first_y, first_z):
    index_x = first_x + jnp.arange(shape[0], dtype=jnp.int32)
    index_y = first_y + jnp.arange(shape[1], dtype=jnp.int32)
    index_z = first_z + jnp.arange(shape[2], dtype=jnp.int32)
    parity = (index_x[:, None, None] + index_y[None, :, None] + index_z[None, None, :]) % 2
    return (parity == 0).astype(jnp.float32)


def black_half(change, target, weights, red_mask, extend, spacing_inv):
    black_mask = 1.0 - red_mask
    return change + black_mask * (jacobian(extend(change), weights, spacing_inv) - target) * weights[6]


def first_sweep(target, weights, red_mask, extend, spacing_inv):
    change = -red_mask * target * weights[6]
    return black_half(change, target, weights, red_mask, extend, spacing_inv)


def full_sweep(change, target, weights, red_mask, extend, spacing_inv):
    change = change + red_mask * (jacobian(extend(change), weights, spacing_inv) - target) * weights[6]
    return black_half(change, target, weights, red_mask, extend, spacing_inv)


def cycle(coarse_level, target, weight_levels, mask_levels):
    spacing_inv = 0.25 ** coarse_level
    weights = weight_levels[coarse_level]
    red_mask = mask_levels[coarse_level]
    change = first_sweep(target, weights, red_mask, wrap_all, spacing_inv)
    if coarse_level == LEVELS - 1:
        for repeat in range(COARSE_SWEEPS - 1):
            change = full_sweep(change, target, weights, red_mask, wrap_all, spacing_inv)
        return change
    leftover = target - jacobian(wrap_all(change), weights, spacing_inv)
    change = change + prolong(cycle(coarse_level + 1, restrict(leftover), weight_levels, mask_levels))
    return full_sweep(change, target, weights, red_mask, wrap_all, spacing_inv)


def reference(density):
    source = density / (jnp.sum(density) / density.size) - 1.0
    potential = jnp.zeros_like(density)
    for newton_step in range(NEWTON):
        weight_levels = []
        mask_levels = []
        coarse = potential
        target = source
        for coarse_level in range(LEVELS):
            if coarse_level > 0:
                coarse = restrict(coarse)
            padded = wrap_all(coarse)
            if coarse_level == 0:
                target = -nonlinear(padded, source)
            weight_levels.append(coefficients(padded, 0.25 ** coarse_level))
            mask_levels.append(checker(coarse.shape, 0, 0, 0))
        potential = potential + cycle(0, target, weight_levels, mask_levels)
    return potential
```

```python
import jax
import jax.numpy as jnp
from jax import lax
from jax.experimental import pallas as pl
from jax.experimental.pallas import tpu as pltpu
from jax.sharding import PartitionSpec as P

NEWTON = 3
COUPLING = 0.1
FLOOR = 3.0
RING = 16
LANES = 128
MESH = pl.DeviceIdType.MESH

HALO = 11
OWN = (12, 8, 12, 6)
SIZE_X = (40, 24, 28, 14)
SIZE_Y = (40, 24, 32, 16)
REACH = 3
BOX1 = [(i, j) for i in (-1, 0, 1) for j in (-1, 0, 1) if (i, j) != (0, 0)]
BOX3 = [
    (i, j)
    for i in range(-REACH, REACH + 1)
    for j in range(-REACH, REACH + 1)
    if (i, j) != (0, 0)
]
LINE_X = [(i, 0) for i in range(1, RING)]
LINE_Y = [(0, j) for j in range(1, RING)]


def rolled(value, shift, axis):
    return pltpu.roll(value, shift % value.shape[axis], axis)


def rows(start, stop, step, body):
    count = (stop - start) // step
    if count == 1:
        for j in range(step):
            body(start + j, j, (start + j) % 2)
    else:

        def chunk(i, carry):
            for j in range(step):
                body(start + i * step + j, j, (start + j) % 2)
            return carry

        lax.fori_loop(0, count, chunk, 0)
    for j in range(count * step, stop - start):
        body(start + j, j, (start + j) % 2)


def neighbours(below, centre, above, stride):
    yp, ym = rolled(centre, -1, 0), rolled(centre, 1, 0)
    zp, zm = rolled(centre, -stride, 1), rolled(centre, stride, 1)
    return above + below, yp + ym, zp + zm, yp - ym


def hessian(below, centre, above, stride):
    sum_x, sum_y, sum_z, diff_y = neighbours(below, centre, above, stride)
    twice = centre + centre
    diff_x = above - below
    mixed_xy = rolled(diff_x, -1, 0) - rolled(diff_x, 1, 0)
    mixed_xz = rolled(diff_x, -stride, 1) - rolled(diff_x, stride, 1)
    mixed_yz = rolled(diff_y, -stride, 1) - rolled(diff_y, stride, 1)
    return sum_x - twice, sum_y - twice, sum_z - twice, mixed_xy, mixed_xz, mixed_yz


def kernel(
    density, out, src, pot0, pot1, pot2, pot3,
    tgt0, tgt1, tgt2, tgt3, pre0, pre1, pre2, pre3,
    va0, va1, va2, va3, vb0, vb1, vb2, vb3,
    co0, co1, co2, co3, fold, packed_t, packed_u, got_t, got_u,
    mean_src, mean_x, mean_y, sends, recvs,
):
    gx, gy = lax.axis_index("gx"), lax.axis_index("gy")
    pot = (pot0, pot1, pot2, pot3)
    tgt = (tgt0, tgt1, tgt2, tgt3)
    pre = (pre0, pre1, pre2, pre3)
    va = (va0, va1, va2, va3)
    vb = (vb0, vb1, vb2, vb3)
    co = (co0, co1, co2, co3)

    def peer(dx, dy):
        return {"gx": lax.rem(gx + dx + RING, RING), "gy": lax.rem(gy + dy + RING, RING)}

    def send(src_ref, dst_ref, which, dx, dy):
        pltpu.make_async_remote_copy(
            src_ref=src_ref,
            dst_ref=dst_ref,
            send_sem=sends.at[which],
            recv_sem=recvs.at[which],
            device_id=peer(dx, dy),
            device_id_type=MESH,
        ).start()

    def finish(ref, sem):
        pltpu.make_async_copy(ref, ref, sem).wait()

    spans = {-1: (0, HALO), 0: (0, 16), 1: (16 - HALO, HALO)}
    lands = {-1: OWN[0] + 16, 0: OWN[0], 1: OWN[0] - HALO}

    def send_halo(src_ref, src_own, dst_ref, which):
        for dx, dy in BOX1:
            sx, nx = spans[dx]
            sy, ny = spans[dy]
            send(
                src_ref.at[pl.ds(src_own + sx, nx), pl.ds(src_own + sy, ny)],
                dst_ref.at[pl.ds(lands[dx], nx), pl.ds(lands[dy], ny)],
                which, dx, dy,
            )

    halo_bytes = co0.at[0, pl.ds(0, 33), pl.ds(0, 36)]

    def send_box(src_ref, dst_ref, which):
        for dx, dy in BOX3:
            at = pl.ds((REACH - dy) * 4, 4)
            if len(src_ref.shape) == 3:
                send(src_ref, dst_ref.at[REACH - dx, :, at], which, dx, dy)
            else:
                send(src_ref, dst_ref.at[REACH - dx, at], which, dx, dy)

    box_t_bytes = co0.at[0, pl.ds(0, 12), pl.ds(0, 32)]
    box_u_bytes = co0.at[0, pl.ds(0, 6), pl.ds(0, 32)]

    def lane_of(shape):
        return lax.broadcasted_iota(jnp.int32, shape, 1)

    def red_masks(level, size, first):
        shape = (size, LANES)
        parity = (
            lax.broadcasted_iota(jnp.int32, shape, 0) + first + (lane_of(shape) >> level)
        ) & 1
        return parity == 0, parity == 1

    def pair_z(value, level):
        stride = 1 << level
        low = ((lane_of(value.shape) >> level) & 1) == 0
        return value + jnp.where(low, rolled(value, -stride, 1), rolled(value, stride, 1))

    barrier = pltpu.get_barrier_semaphore()
    everyone = sorted(set(BOX3 + [(i - RING if i > 8 else i, 0) for i in range(1, RING)]
                          + [(0, j - RING if j > 8 else j) for j in range(1, RING)]))
    for dx, dy in everyone:
        pl.semaphore_signal(barrier, inc=1, device_id=peer(dx, dy), device_id_type=MESH)

    total = density[0]
    for x in range(1, 16):
        total = total + density[x]
    mean_src[0] = jnp.sum(total, axis=0, keepdims=True)
    mean_x[gx] = mean_src[0]

    def clear(x, j, parity):
        pot0[x] = jnp.zeros(pot0.shape[1:], jnp.float32)

    rows(0, SIZE_X[0], 4, clear)

    def clear2(x, j, parity):
        pot2[x] = jnp.zeros(pot2.shape[1:], jnp.float32)

    rows(0, SIZE_X[2], 4, clear2)
    pl.semaphore_wait(barrier, len(everyone))

    for dx, dy in LINE_X:
        send(mean_src.at[0], mean_x.at[gx], 0, dx, dy)
    send_halo(density, 0, src, 1)
    own = pl.ds(OWN[0], 16)

    def copy_own(x, j, parity):
        src[OWN[0] + x, own] = density[x]

    rows(0, 16, 4, copy_own)
    fifteen = mean_x.at[pl.ds(0, RING - 1)]
    finish(fifteen, recvs.at[0])
    row = mean_x[0]
    for i in range(1, RING):
        row = row + mean_x[i]
    mean_src[1] = row
    mean_y[gy] = row
    for dx, dy in LINE_Y:
        send(mean_src.at[1], mean_y.at[gy], 2, dx, dy)
    finish(fifteen, recvs.at[2])
    row = mean_y[0]
    for i in range(1, RING):
        row = row + mean_y[i]
    cells = RING * RING * 16 * 16 * LANES
    mean = jnp.sum(row, axis=1, keepdims=True) * (1.0 / cells)
    finish(halo_bytes, recvs.at[1])
    finish(fifteen, sends.at[0])
    finish(fifteen, sends.at[2])
    finish(halo_bytes, sends.at[1])

    def to_source(x, j, parity):
        src[x] = src[x] / mean - 1.0

    rows(1, 39, 2, to_source)

    def coefficients(level, start, stop, step, with_target=False):
        inv = 0.25**level
        field = pot[level]
        store = co[level]

        def body(x, j, parity):
            xx, yy, zz, xy, xz, yz = hessian(field[x - 1], field[x], field[x + 1], 1 << level)
            if level:
                xx, yy, zz = xx * inv, yy * inv, zz * inv
            quarter = 0.25 * inv
            stiff_x = 1.0 + 2.0 * COUPLING * (yy + zz)
            stiff_y = 1.0 + 2.0 * COUPLING * (xx + zz)
            stiff_z = 1.0 + 2.0 * COUPLING * (xx + yy)
            diagonal = jnp.maximum(2.0 * (stiff_x + stiff_y + stiff_z), FLOOR)
            relax = (1.0 / inv) / diagonal
            if level:
                store[0, x], store[1, x], store[2, x] = stiff_x * inv, stiff_y * inv, stiff_z * inv
            else:
                store[0, x], store[1, x], store[2, x] = stiff_x, stiff_y, stiff_z
            weight = -4.0 * COUPLING * quarter * quarter
            store[3, x], store[4, x], store[5, x] = xy * weight, xz * weight, yz * weight
            store[6, x] = relax
            if with_target:
                cubic = xx * yy + xx * zz + yy * zz - (xy * xy + xz * xz + yz * yz) * 0.0625
                target = src[x] - (xx + yy + zz + 2.0 * COUPLING * cubic)
                tgt[level][x] = target
                pre[level][x] = -target * relax

        rows(start, stop, step, body)

    def jacobian(level, field, x, ys):
        parts = hessian(field[x - 1, ys], field[x, ys], field[x + 1, ys], 1 << level)
        store = co[level]
        result = store[0, x, ys] * parts[0]
        for index in range(1, 6):
            result = result + store[index, x, ys] * parts[index]
        return result

    def whole(level):
        return pl.ds(0, SIZE_Y[level])

    def first_sweep(level, start, stop, step):
        masks = red_masks(level, SIZE_Y[level], 0)
        field, store = pre[level], co[level]

        def body(x, j, parity):
            centre = field[x]
            sum_x, sum_y, sum_z, _ = neighbours(field[x - 1], centre, field[x + 1], 1 << level)
            spread = store[0, x] * sum_x + store[1, x] * sum_y + store[2, x] * sum_z
            va[level][x] = jnp.where(masks[parity], centre, centre + spread * store[6, x])

        rows(start, stop, step, body)

    def half_sweep(level, colour, start, stop, step, ys, sink=None):
        masks = red_masks(level, ys.size, ys.start)
        from_ref, to_ref = (va, vb) if colour == 0 else (vb, va)
        from_ref, to_ref = from_ref[level], to_ref[level]

        def body(x, j, parity):
            old = from_ref[x, ys]
            change = (jacobian(level, from_ref, x, ys) - tgt[level][x, ys]) * co[level][6, x, ys]
            new = jnp.where(masks[(parity + colour) % 2], old + change, old)
            if sink is None:
                to_ref[x, ys] = new
            else:
                sink(x, new)

        rows(start, stop, step, body)

    def restricted(level, start, stop, pairs, first, count, sink):
        first_x, first_y = first

        def body(x, j, parity):
            fine = first_x + 2 * x
            acc = None
            for k in range(2):
                left = tgt[level][fine + k] - jacobian(level, va[level], fine + k, whole(level))
                acc = left if acc is None else acc + left
            slot = fold.at[j]
            slot[pl.ds(0, SIZE_Y[level]), :] = pair_z(acc, level)
            sink(x, 0.125 * (slot[pl.ds(first_y, count, 2), :] + slot[pl.ds(first_y + 1, count, 2), :]))

        rows(start, stop, pairs, body)

    def averaged(level, fine, first_y, count):
        field = pot[level]
        acc = None
        for k in range(2):
            for q in range(2):
                part = field[fine + k, pl.ds(first_y + q, count, 2), :]
                acc = part if acc is None else acc + part
        return 0.125 * pair_z(acc, level)

    def prolonged(level, start, stop, step, first_y, count, coarse_of, coarse_y):
        fine_ref, coarse_ref = va[level], va[level + 1]

        def body(x, j, parity):
            value = coarse_ref[x, pl.ds(coarse_y, count)]
            for k in range(2):
                for q in range(2):
                    at = (coarse_of(x) + k, pl.ds(first_y + q, count, 2), slice(None))
                    fine_ref[at] = fine_ref[at] + value

        rows(start, stop, step, body)

    quad = lane_of((4, LANES)) & 3

    def pack(values):
        return jnp.where(
            quad == 0, values[0], jnp.where(quad == 1, values[1], jnp.where(quad == 2, values[2], values[3]))
        )

    def unpack(read, write):
        place = lane_of((28, LANES)) & 3

        def body(g, j, parity):
            value = read(g)
            turned = {d: (value if d == 0 else rolled(value, -d, 1)) for d in range(-3, 4)}
            for i in range(4):
                piece = turned[i - 3]
                for k in (2, 1, 0):
                    piece = jnp.where(place == k, turned[i - k], piece)
                write(4 * g + i, piece)

        rows(0, 2 * REACH + 1, 1, body)

    def newton(step, carry):
        def coarse1(x, j, parity):
            pot1[x, pl.ds(2, 20)] = averaged(0, 2 * x - 4, 0, 20)

        rows(3, 21, 2, coarse1)
        coefficients(0, 2, 38, 2, with_target=True)
        coefficients(1, 4, 20, 2)
        coefficients(2, 12, 16, 2)
        first_sweep(0, 3, 37, 2)

        def to_level1(x, value):
            tgt1[4 + x, pl.ds(4, 16)] = value
            pre1[4 + x, pl.ds(4, 16)] = -value * co1[6, 4 + x, pl.ds(4, 16)]

        restricted(0, 0, 16, 2, (4, 4), 16, to_level1)
        first_sweep(1, 5, 19, 2)
        kept = []

        def to_level2(x, value):
            kept.append((value, -value * co2[6, 12 + x, pl.ds(12, 4)]))

        restricted(1, 0, 4, 4, (8, 8), 4, to_level2)
        packed_t[0] = pack([k[0] for k in kept])
        packed_t[1] = pack([k[1] for k in kept])
        send_box(packed_t, got_t, 3)
        for q in range(2):
            got_t[REACH, q, pl.ds(12, 4)] = packed_t[q]
        coefficients(2, 1, 12, 1)
        coefficients(2, 16, 27, 1)

        def coarse3(x, j, parity):
            pot3[x] = averaged(2, 2 * x, 0, 16)

        rows(0, 14, 2, coarse3)
        coefficients(3, 1, 13, 2)
        finish(box_t_bytes, recvs.at[3])

        def put(ref):
            def write(x, value):
                ref[x, pl.ds(0, 28)] = value

            return write

        unpack(lambda g: got_t[g, 0], put(tgt2))
        unpack(lambda g: got_t[g, 1], put(pre2))
        first_sweep(2, 1, 27, 2)

        def to_level3(x, value):
            tgt3[1 + x] = value
            pre3[1 + x] = -value * co3[6, 1 + x]

        restricted(2, 0, 12, 2, (2, 0), 16, to_level3)
        first_sweep(3, 2, 12, 2)
        half_sweep(3, 0, 3, 11, 2, whole(3))
        half_sweep(3, 1, 4, 10, 2, whole(3))
        prolonged(2, 4, 10, 2, 8, 6, lambda x: 2 * x, 4)
        half_sweep(2, 0, 9, 19, 2, pl.ds(8, 16))
        half_sweep(2, 1, 10, 18, 2, pl.ds(8, 16))
        prolonged(1, 10, 18, 2, 4, 8, lambda x: 2 * x - 16, 10)
        half_sweep(1, 0, 6, 18, 2, whole(1))
        half_sweep(1, 1, 7, 17, 2, whole(1))
        prolonged(0, 7, 17, 2, 10, 10, lambda x: 2 * x - 4, 7)
        half_sweep(0, 0, 11, 29, 2, pl.ds(8, 24))

        def add_own(x, new):
            pot0[x, own] = pot0[x, own] + new[4:20]

        half_sweep(0, 1, 12, 28, 2, pl.ds(8, 24), sink=add_own)
        finish(box_t_bytes, sends.at[3])

        @pl.when(step < NEWTON - 1)
        def _():
            send_halo(pot0, OWN[0], pot0, 1)

            def own1(x, j, parity):
                pot1[x, pl.ds(8, 8)] = averaged(0, 2 * x - 4, 12, 8)

            rows(8, 16, 4, own1)
            packed_u[...] = pack([averaged(1, 8 + 2 * x, 8, 4) for x in range(4)])
            send_box(packed_u, got_u, 4)
            got_u[REACH, pl.ds(12, 4)] = packed_u[...]
            finish(box_u_bytes, recvs.at[4])
            unpack(lambda g: got_u[g], put(pot2))
            finish(halo_bytes, recvs.at[1])
            finish(halo_bytes, sends.at[1])
            finish(box_u_bytes, sends.at[4])

        return carry

    lax.fori_loop(0, NEWTON, newton, 0)

    def result(x, j, parity):
        out[x] = pot0[OWN[0] + x, own]

    rows(0, 16, 4, result)


def per_device(density):
    def fields(count):
        return [
            pltpu.VMEM((SIZE_X[level], SIZE_Y[level], LANES), jnp.float32)
            for _ in range(count)
            for level in range(4)
        ]

    pots, tgts, pres, vas, vbs = (fields(1) for _ in range(5))
    cos = [pltpu.VMEM((7, SIZE_X[level], SIZE_Y[level], LANES), jnp.float32) for level in range(4)]
    return pl.pallas_call(
        kernel,
        out_shape=jax.ShapeDtypeStruct(density.shape, jnp.float32),
        in_specs=[pl.BlockSpec(memory_space=pltpu.VMEM)],
        out_specs=pl.BlockSpec(memory_space=pltpu.VMEM),
        scratch_shapes=[
            pltpu.VMEM((SIZE_X[0], SIZE_Y[0], LANES), jnp.float32),
            *pots, *tgts, *pres, *vas, *vbs, *cos,
            pltpu.VMEM((4, 40, LANES), jnp.float32),
            pltpu.VMEM((2, 4, LANES), jnp.float32),
            pltpu.VMEM((4, LANES), jnp.float32),
            pltpu.VMEM((7, 2, 28, LANES), jnp.float32),
            pltpu.VMEM((7, 28, LANES), jnp.float32),
            pltpu.VMEM((2, 1, LANES), jnp.float32),
            pltpu.VMEM((RING, 1, LANES), jnp.float32),
            pltpu.VMEM((RING, 1, LANES), jnp.float32),
            pltpu.SemaphoreType.DMA((5,)),
            pltpu.SemaphoreType.DMA((5,)),
        ],
        compiler_params=pltpu.CompilerParams(collective_id=0, has_side_effects=True),
    )(density)


def solution(mesh):
    return jax.shard_map(
        per_device,
        mesh=mesh,
        in_specs=(P("gx", "gy", None),),
        out_specs=P("gx", "gy", None),
        check_vma=False,
    )
```

```python
import jax
import jax.numpy as jnp
from jax import lax
from jax.experimental import pallas as pl
from jax.experimental.pallas import tpu as pltpu
from jax.sharding import PartitionSpec as P

NEWTON = 3
COUPLING = 0.1
FLOOR = 3.0
RING = 16
LANES = 128
MESH = pl.DeviceIdType.MESH

HALO = 11
OWN = (12, 8, 12, 6)
SIZE_X = (40, 24, 28, 14)
SIZE_Y = (40, 24, 32, 16)
STEP = dict(coarse1=18, a0=12, a1=8, b0=34, c0=4, b1=14, a2=11, coarse3=14, a3=12, b2=26, c2=6, b3=10, e3=8, f3=6,
            e2=10, f2=8, e1=12, f1=10, e0=18, f0=16, d2=6, d1=8, d0=10, un=7)
REACH = 3
BOX1 = [(i, j) for i in (-1, 0, 1) for j in (-1, 0, 1) if (i, j) != (0, 0)]
BOX3 = [
    (i, j)
    for i in range(-REACH, REACH + 1)
    for j in range(-REACH, REACH + 1)
    if (i, j) != (0, 0)
]
LINE_X = [(i, 0) for i in range(1, RING)]
LINE_Y = [(0, j) for j in range(1, RING)]


def rolled(value, shift, axis):
    return pltpu.roll(value, shift % value.shape[axis], axis)


def rows(start, stop, step, body):
    count = (stop - start) // step
    if count == 1:
        for j in range(step):
            body(start + j, j, (start + j) % 2)
    else:
        assert step % 2 == 0 or step == 1

        def chunk(i, carry):
            for j in range(step):
                body(start + i * step + j, j, (start + j) % 2)
            return carry

        lax.fori_loop(0, count, chunk, 0)
    for j in range(count * step, stop - start):
        body(start + j, j, (start + j) % 2)


def neighbours(below, centre, above, stride):
    yp, ym = rolled(centre, -1, 0), rolled(centre, 1, 0)
    zp, zm = rolled(centre, -stride, 1), rolled(centre, stride, 1)
    return above + below, yp + ym, zp + zm, yp - ym


def hessian(below, centre, above, stride):
    sum_x, sum_y, sum_z, diff_y = neighbours(below, centre, above, stride)
    twice = centre + centre
    diff_x = above - below
    mixed_xy = rolled(diff_x, -1, 0) - rolled(diff_x, 1, 0)
    mixed_xz = rolled(diff_x, -stride, 1) - rolled(diff_x, stride, 1)
    mixed_yz = rolled(diff_y, -stride, 1) - rolled(diff_y, stride, 1)
    return sum_x - twice, sum_y - twice, sum_z - twice, mixed_xy, mixed_xz, mixed_yz


def kernel(
    density, out, src, pot0, pot1, pot2, pot3,
    tgt0, tgt1, tgt2, tgt3, pre0, pre1, pre2, pre3,
    va0, va1, va2, va3, vb0, vb1, vb2, vb3,
    co0, co1, co2, co3, fold, packed_t, packed_u, got_t, got_u,
    mean_src, mean_x, mean_y, sends, recvs,
):
    gx, gy = lax.axis_index("gx"), lax.axis_index("gy")
    pot = (pot0, pot1, pot2, pot3)
    tgt = (tgt0, tgt1, tgt2, tgt3)
    pre = (pre0, pre1, pre2, pre3)
    va = (va0, va1, va2, va3)
    vb = (vb0, vb1, vb2, vb3)
    co = (co0, co1, co2, co3)

    def peer(dx, dy):
        return {"gx": lax.rem(gx + dx + RING, RING), "gy": lax.rem(gy + dy + RING, RING)}

    def send(src_ref, dst_ref, which, dx, dy):
        pltpu.make_async_remote_copy(
            src_ref=src_ref,
            dst_ref=dst_ref,
            send_sem=sends.at[which],
            recv_sem=recvs.at[which],
            device_id=peer(dx, dy),
            device_id_type=MESH,
        ).start()

    def finish(ref, sem):
        pltpu.make_async_copy(ref, ref, sem).wait()

    spans = {-1: (0, HALO), 0: (0, 16), 1: (16 - HALO, HALO)}
    lands = {-1: OWN[0] + 16, 0: OWN[0], 1: OWN[0] - HALO}

    def send_halo(src_ref, src_own, dst_ref, which):
        for dx, dy in BOX1:
            sx, nx = spans[dx]
            sy, ny = spans[dy]
            send(
                src_ref.at[pl.ds(src_own + sx, nx), pl.ds(src_own + sy, ny)],
                dst_ref.at[pl.ds(lands[dx], nx), pl.ds(lands[dy], ny)],
                which, dx, dy,
            )

    halo_bytes = co0.at[0, pl.ds(0, 33), pl.ds(0, 36)]

    def send_box(src_ref, dst_ref, which):
        for dx, dy in BOX3:
            at = pl.ds((REACH - dy) * 4, 4)
            if len(src_ref.shape) == 3:
                send(src_ref, dst_ref.at[REACH - dx, :, at], which, dx, dy)
            else:
                send(src_ref, dst_ref.at[REACH - dx, at], which, dx, dy)

    box_t_bytes = co0.at[0, pl.ds(0, 12), pl.ds(0, 32)]
    box_u_bytes = co0.at[0, pl.ds(0, 6), pl.ds(0, 32)]

    def lane_of(shape):
        return lax.broadcasted_iota(jnp.int32, shape, 1)

    def red_masks(level, size, first):
        shape = (size, LANES)
        parity = (
            lax.broadcasted_iota(jnp.int32, shape, 0) + first + (lane_of(shape) >> level)
        ) & 1
        return parity == 0, parity == 1

    def pair_z(value, level):
        stride = 1 << level
        low = ((lane_of(value.shape) >> level) & 1) == 0
        return value + jnp.where(low, rolled(value, -stride, 1), rolled(value, stride, 1))

    barrier = pltpu.get_barrier_semaphore()
    everyone = sorted(set(BOX3 + [(i - RING if i > 8 else i, 0) for i in range(1, RING)]
                          + [(0, j - RING if j > 8 else j) for j in range(1, RING)]))
    for dx, dy in everyone:
        pl.semaphore_signal(barrier, inc=1, device_id=peer(dx, dy), device_id_type=MESH)

    total = density[0]
    for x in range(1, 16):
        total = total + density[x]
    mean_src[0] = jnp.sum(total, axis=0, keepdims=True)
    mean_x[gx] = mean_src[0]

    def clear(x, j, parity):
        pot0[x] = jnp.zeros(pot0.shape[1:], jnp.float32)

    rows(0, SIZE_X[0], 4, clear)

    def clear2(x, j, parity):
        pot2[x] = jnp.zeros(pot2.shape[1:], jnp.float32)

    rows(0, SIZE_X[2], 4, clear2)
    pl.semaphore_wait(barrier, len(everyone))

    for dx, dy in LINE_X:
        send(mean_src.at[0], mean_x.at[gx], 0, dx, dy)
    send_halo(density, 0, src, 1)
    own = pl.ds(OWN[0], 16)

    def copy_own(x, j, parity):
        src[OWN[0] + x, own] = density[x]

    rows(0, 16, 4, copy_own)
    fifteen = mean_x.at[pl.ds(0, RING - 1)]
    finish(fifteen, recvs.at[0])
    row = mean_x[0]
    for i in range(1, RING):
        row = row + mean_x[i]
    mean_src[1] = row
    mean_y[gy] = row
    for dx, dy in LINE_Y:
        send(mean_src.at[1], mean_y.at[gy], 2, dx, dy)
    finish(fifteen, recvs.at[2])
    row = mean_y[0]
    for i in range(1, RING):
        row = row + mean_y[i]
    cells = RING * RING * 16 * 16 * LANES
    mean = jnp.sum(row, axis=1, keepdims=True) * (1.0 / cells)
    finish(halo_bytes, recvs.at[1])
    finish(fifteen, sends.at[0])
    finish(fifteen, sends.at[2])
    finish(halo_bytes, sends.at[1])

    def to_source(x, j, parity):
        src[x] = src[x] / mean - 1.0

    rows(1, 39, 2, to_source)

    def coefficients(level, start, stop, step, with_target=False):
        inv = 0.25**level
        field = pot[level]
        store = co[level]

        def body(x, j, parity):
            xx, yy, zz, xy, xz, yz = hessian(field[x - 1], field[x], field[x + 1], 1 << level)
            if level:
                xx, yy, zz = xx * inv, yy * inv, zz * inv
            quarter = 0.25 * inv
            stiff_x = 1.0 + 2.0 * COUPLING * (yy + zz)
            stiff_y = 1.0 + 2.0 * COUPLING * (xx + zz)
            stiff_z = 1.0 + 2.0 * COUPLING * (xx + yy)
            diagonal = jnp.maximum(2.0 * (stiff_x + stiff_y + stiff_z), FLOOR)
            relax = (1.0 / inv) / diagonal
            if level:
                store[0, x], store[1, x], store[2, x] = stiff_x * inv, stiff_y * inv, stiff_z * inv
            else:
                store[0, x], store[1, x], store[2, x] = stiff_x, stiff_y, stiff_z
            weight = -4.0 * COUPLING * quarter * quarter
            store[3, x], store[4, x], store[5, x] = xy * weight, xz * weight, yz * weight
            store[6, x] = relax
            if with_target:
                cubic = xx * yy + xx * zz + yy * zz - (xy * xy + xz * xz + yz * yz) * 0.0625
                target = src[x] - (xx + yy + zz + 2.0 * COUPLING * cubic)
                tgt[level][x] = target
                pre[level][x] = -target * relax

        rows(start, stop, step, body)

    def jacobian(level, field, x, ys):
        parts = hessian(field[x - 1, ys], field[x, ys], field[x + 1, ys], 1 << level)
        store = co[level]
        result = store[0, x, ys] * parts[0]
        for index in range(1, 6):
            result = result + store[index, x, ys] * parts[index]
        return result

    def whole(level):
        return pl.ds(0, SIZE_Y[level])

    def first_sweep(level, start, stop, step):
        masks = red_masks(level, SIZE_Y[level], 0)
        field, store = pre[level], co[level]

        def body(x, j, parity):
            centre = field[x]
            sum_x, sum_y, sum_z, _ = neighbours(field[x - 1], centre, field[x + 1], 1 << level)
            spread = store[0, x] * sum_x + store[1, x] * sum_y + store[2, x] * sum_z
            va[level][x] = jnp.where(masks[parity], centre, centre + spread * store[6, x])

        rows(start, stop, step, body)

    def half_sweep(level, colour, start, stop, step, ys, sink=None):
        masks = red_masks(level, ys.size, ys.start)
        from_ref, to_ref = (va, vb) if colour == 0 else (vb, va)
        from_ref, to_ref = from_ref[level], to_ref[level]

        def body(x, j, parity):
            old = from_ref[x, ys]
            change = (jacobian(level, from_ref, x, ys) - tgt[level][x, ys]) * co[level][6, x, ys]
            new = jnp.where(masks[(parity + colour) % 2], old + change, old)
            if sink is None:
                to_ref[x, ys] = new
            else:
                sink(x, new)

        rows(start, stop, step, body)

    def restricted(level, start, stop, pairs, first, count, sink):
        first_x, first_y = first

        def body(x, j, parity):
            fine = first_x + 2 * x
            acc = None
            for k in range(2):
                left = tgt[level][fine + k] - jacobian(level, va[level], fine + k, whole(level))
                acc = left if acc is None else acc + left
            slot = fold.at[j]
            slot[pl.ds(0, SIZE_Y[level]), :] = pair_z(acc, level)
            sink(x, 0.125 * (slot[pl.ds(first_y, count, 2), :] + slot[pl.ds(first_y + 1, count, 2), :]))

        rows(start, stop, pairs, body)

    def averaged(level, fine, first_y, count):
        field = pot[level]
        acc = None
        for k in range(2):
            for q in range(2):
                part = field[fine + k, pl.ds(first_y + q, count, 2), :]
                acc = part if acc is None else acc + part
        return 0.125 * pair_z(acc, level)

    def prolonged(level, start, stop, step, first_y, count, coarse_of, coarse_y):
        fine_ref, coarse_ref = va[level], va[level + 1]

        def body(x, j, parity):
            value = coarse_ref[x, pl.ds(coarse_y, count)]
            for k in range(2):
                for q in range(2):
                    at = (coarse_of(x) + k, pl.ds(first_y + q, count, 2), slice(None))
                    fine_ref[at] = fine_ref[at] + value

        rows(start, stop, step, body)

    quad = lane_of((4, LANES)) & 3

    def pack(values):
        return jnp.where(
            quad == 0, values[0], jnp.where(quad == 1, values[1], jnp.where(quad == 2, values[2], values[3]))
        )

    def unpack(read, write):
        place = lane_of((28, LANES)) & 3

        def body(g, j, parity):
            value = read(g)
            turned = {d: (value if d == 0 else rolled(value, -d, 1)) for d in range(-3, 4)}
            for i in range(4):
                piece = turned[i - 3]
                for k in (2, 1, 0):
                    piece = jnp.where(place == k, turned[i - k], piece)
                write(4 * g + i, piece)

        rows(0, 2 * REACH + 1, STEP['un'], body)

    def newton(step, carry):
        def coarse1(x, j, parity):
            pot1[x, pl.ds(2, 20)] = averaged(0, 2 * x - 4, 0, 20)

        rows(3, 21, STEP['coarse1'], coarse1)
        coefficients(0, 2, 38, STEP['a0'], with_target=True)
        coefficients(1, 4, 20, STEP['a1'])
        coefficients(2, 12, 16, 4)
        first_sweep(0, 3, 37, STEP['b0'])

        def to_level1(x, value):
            tgt1[4 + x, pl.ds(4, 16)] = value
            pre1[4 + x, pl.ds(4, 16)] = -value * co1[6, 4 + x, pl.ds(4, 16)]

        restricted(0, 0, 16, STEP['c0'], (4, 4), 16, to_level1)
        first_sweep(1, 5, 19, STEP['b1'])
        kept = []

        def to_level2(x, value):
            kept.append((value, -value * co2[6, 12 + x, pl.ds(12, 4)]))

        restricted(1, 0, 4, 4, (8, 8), 4, to_level2)
        packed_t[0] = pack([k[0] for k in kept])
        packed_t[1] = pack([k[1] for k in kept])
        send_box(packed_t, got_t, 3)
        for q in range(2):
            got_t[REACH, q, pl.ds(12, 4)] = packed_t[q]
        coefficients(2, 1, 12, STEP['a2'])
        coefficients(2, 16, 27, STEP['a2'])

        def coarse3(x, j, parity):
            pot3[x] = averaged(2, 2 * x, 0, 16)

        rows(0, 14, STEP['coarse3'], coarse3)
        coefficients(3, 1, 13, STEP['a3'])
        finish(box_t_bytes, recvs.at[3])

        def put(ref):
            def write(x, value):
                ref[x, pl.ds(0, 28)] = value

            return write

        unpack(lambda g: got_t[g, 0], put(tgt2))
        unpack(lambda g: got_t[g, 1], put(pre2))
        first_sweep(2, 1, 27, STEP['b2'])

        def to_level3(x, value):
            tgt3[1 + x] = value
            pre3[1 + x] = -value * co3[6, 1 + x]

        restricted(2, 0, 12, STEP['c2'], (2, 0), 16, to_level3)
        first_sweep(3, 2, 12, STEP['b3'])
        half_sweep(3, 0, 3, 11, STEP['e3'], whole(3))
        half_sweep(3, 1, 4, 10, STEP['f3'], whole(3))
        prolonged(2, 4, 10, STEP['d2'], 8, 6, lambda x: 2 * x, 4)
        half_sweep(2, 0, 9, 19, STEP['e2'], pl.ds(8, 16))
        half_sweep(2, 1, 10, 18, STEP['f2'], pl.ds(8, 16))
        prolonged(1, 10, 18, STEP['d1'], 4, 8, lambda x: 2 * x - 16, 10)
        half_sweep(1, 0, 6, 18, STEP['e1'], whole(1))
        half_sweep(1, 1, 7, 17, STEP['f1'], whole(1))
        prolonged(0, 7, 17, STEP['d0'], 10, 10, lambda x: 2 * x - 4, 7)
        half_sweep(0, 0, 11, 29, STEP['e0'], pl.ds(8, 24))

        def add_own(x, new):
            pot0[x, own] = pot0[x, own] + new[4:20]

        half_sweep(0, 1, 12, 28, STEP['f0'], pl.ds(8, 24), sink=add_own)
        finish(box_t_bytes, sends.at[3])

        @pl.when(step < NEWTON - 1)
        def _():
            send_halo(pot0, OWN[0], pot0, 1)

            def own1(x, j, parity):
                pot1[x, pl.ds(8, 8)] = averaged(0, 2 * x - 4, 12, 8)

            rows(8, 16, 4, own1)
            packed_u[...] = pack([averaged(1, 8 + 2 * x, 8, 4) for x in range(4)])
            send_box(packed_u, got_u, 4)
            got_u[REACH, pl.ds(12, 4)] = packed_u[...]
            finish(box_u_bytes, recvs.at[4])
            unpack(lambda g: got_u[g], put(pot2))
            finish(halo_bytes, recvs.at[1])
            finish(halo_bytes, sends.at[1])
            finish(box_u_bytes, sends.at[4])

        return carry

    lax.fori_loop(0, NEWTON, newton, 0)

    def result(x, j, parity):
        out[x] = pot0[OWN[0] + x, own]

    rows(0, 16, 4, result)


def per_device(density):
    def fields(count):
        return [
            pltpu.VMEM((SIZE_X[level], SIZE_Y[level], LANES), jnp.float32)
            for _ in range(count)
            for level in range(4)
        ]

    pots, tgts, pres, vas, vbs = (fields(1) for _ in range(5))
    cos = [pltpu.VMEM((7, SIZE_X[level], SIZE_Y[level], LANES), jnp.float32) for level in range(4)]
    return pl.pallas_call(
        kernel,
        out_shape=jax.ShapeDtypeStruct(density.shape, jnp.float32),
        in_specs=[pl.BlockSpec(memory_space=pltpu.VMEM)],
        out_specs=pl.BlockSpec(memory_space=pltpu.VMEM),
        scratch_shapes=[
            pltpu.VMEM((SIZE_X[0], SIZE_Y[0], LANES), jnp.float32),
            *pots, *tgts, *pres, *vas, *vbs, *cos,
            pltpu.VMEM((16, 40, LANES), jnp.float32),
            pltpu.VMEM((2, 4, LANES), jnp.float32),
            pltpu.VMEM((4, LANES), jnp.float32),
            pltpu.VMEM((7, 2, 28, LANES), jnp.float32),
            pltpu.VMEM((7, 28, LANES), jnp.float32),
            pltpu.VMEM((2, 1, LANES), jnp.float32),
            pltpu.VMEM((RING, 1, LANES), jnp.float32),
            pltpu.VMEM((RING, 1, LANES), jnp.float32),
            pltpu.SemaphoreType.DMA((5,)),
            pltpu.SemaphoreType.DMA((5,)),
        ],
        compiler_params=pltpu.CompilerParams(collective_id=0, has_side_effects=True),
    )(density)


def solution(mesh):
    return jax.shard_map(
        per_device,
        mesh=mesh,
        in_specs=(P("gx", "gy", None),),
        out_specs=P("gx", "gy", None),
        check_vma=False,
    )
```

```python
import jax
import jax.numpy as jnp
from jax import lax
from jax.experimental import pallas as pl
from jax.experimental.pallas import tpu as pltpu
from jax.sharding import PartitionSpec as P

NEWTON = 3
COUPLING = 0.1
FLOOR = 3.0
RING = 16
LANES = 128
MESH = pl.DeviceIdType.MESH

HALO = 11
OWN = (12, 8, 12, 6)
SIZE_X = (40, 24, 28, 14)
SIZE_Y = (40, 24, 32, 16)
STEP = dict(coarse1=18, a0=12, a1=8, b0=34, c0=4, b1=14, a2=26, coarse3=14, a3=12, b2=26, c2=6, b3=10, e3=8, f3=6,
            e2=10, f2=8, e1=12, f1=10, e0=18, f0=16, d2=6, d1=8, d0=10, un=7)
REACH = 3
BOX1 = [(i, j) for i in (-1, 0, 1) for j in (-1, 0, 1) if (i, j) != (0, 0)]
BOX3 = [
    (i, j)
    for i in range(-REACH, REACH + 1)
    for j in range(-REACH, REACH + 1)
    if (i, j) != (0, 0)
]
LINE_X = [(i, 0) for i in range(1, RING)]
LINE_Y = [(0, j) for j in range(1, RING)]


def rolled(value, shift, axis):
    return pltpu.roll(value, shift % value.shape[axis], axis)


def rows(start, stop, step, body):
    count = (stop - start) // step
    if count == 1:
        for j in range(step):
            body(start + j, j, (start + j) % 2)
    else:
        assert step % 2 == 0 or step == 1

        def chunk(i, carry):
            for j in range(step):
                body(start + i * step + j, j, (start + j) % 2)
            return carry

        lax.fori_loop(0, count, chunk, 0)
    for j in range(count * step, stop - start):
        body(start + j, j, (start + j) % 2)


def neighbours(below, centre, above, stride):
    yp, ym = rolled(centre, -1, 0), rolled(centre, 1, 0)
    zp, zm = rolled(centre, -stride, 1), rolled(centre, stride, 1)
    return above + below, yp + ym, zp + zm, yp - ym


def hessian(below, centre, above, stride):
    sum_x, sum_y, sum_z, diff_y = neighbours(below, centre, above, stride)
    twice = centre + centre
    diff_x = above - below
    mixed_xy = rolled(diff_x, -1, 0) - rolled(diff_x, 1, 0)
    mixed_xz = rolled(diff_x, -stride, 1) - rolled(diff_x, stride, 1)
    mixed_yz = rolled(diff_y, -stride, 1) - rolled(diff_y, stride, 1)
    return sum_x - twice, sum_y - twice, sum_z - twice, mixed_xy, mixed_xz, mixed_yz


def kernel(
    density, out, src, pot0, pot1, pot2, pot3,
    tgt0, tgt1, tgt2, tgt3, pre0, pre1, pre2, pre3,
    va0, va1, va2, va3, vb0, vb1, vb2, vb3,
    co0, co1, co2, co3, fold, packed_t, packed_u, got_0, got_t, got_u,
    mean_src, mean_x, mean_y, sends, recvs,
):
    gx, gy = lax.axis_index("gx"), lax.axis_index("gy")
    pot = (pot0, pot1, pot2, pot3)
    tgt = (tgt0, tgt1, tgt2, tgt3)
    pre = (pre0, pre1, pre2, pre3)
    va = (va0, va1, va2, va3)
    vb = (vb0, vb1, vb2, vb3)
    co = (co0, co1, co2, co3)

    def peer(dx, dy):
        return {"gx": lax.rem(gx + dx + RING, RING), "gy": lax.rem(gy + dy + RING, RING)}

    def send(src_ref, dst_ref, which, dx, dy):
        pltpu.make_async_remote_copy(
            src_ref=src_ref,
            dst_ref=dst_ref,
            send_sem=sends.at[which],
            recv_sem=recvs.at[which],
            device_id=peer(dx, dy),
            device_id_type=MESH,
        ).start()

    def finish(ref, sem):
        pltpu.make_async_copy(ref, ref, sem).wait()

    spans = {-1: (0, HALO), 0: (0, 16), 1: (16 - HALO, HALO)}
    lands = {-1: OWN[0] + 16, 0: OWN[0], 1: OWN[0] - HALO}

    def send_halo(src_ref, src_own, dst_ref, side, rest):
        for dx, dy in [(0, 1), (0, -1)] + [o for o in BOX1 if o[0]]:
            sx, nx = spans[dx]
            sy, ny = spans[dy]
            send(
                src_ref.at[pl.ds(src_own + sx, nx), pl.ds(src_own + sy, ny)],
                dst_ref.at[pl.ds(lands[dx], nx), pl.ds(lands[dy], ny)],
                rest if dx else side, dx, dy,
            )

    halo_bytes = co0.at[0, pl.ds(0, 33), pl.ds(0, 36)]
    side_bytes = co0.at[0, pl.ds(0, 11), pl.ds(0, 32)]
    rest_bytes = co0.at[0, pl.ds(0, 38), pl.ds(0, 22)]

    def send_box(src_ref, dst_ref, which):
        for dx, dy in BOX3:
            at = pl.ds((REACH - dy) * 4, 4)
            if len(src_ref.shape) == 3:
                send(src_ref, dst_ref.at[REACH - dx, :, at], which, dx, dy)
            else:
                send(src_ref, dst_ref.at[REACH - dx, at], which, dx, dy)

    box_t_bytes = co0.at[0, pl.ds(0, 12), pl.ds(0, 32)]
    box_u_bytes = co0.at[0, pl.ds(0, 6), pl.ds(0, 32)]

    def lane_of(shape):
        return lax.broadcasted_iota(jnp.int32, shape, 1)

    def red_masks(level, size, first):
        shape = (size, LANES)
        parity = (
            lax.broadcasted_iota(jnp.int32, shape, 0) + first + (lane_of(shape) >> level)
        ) & 1
        return parity == 0, parity == 1

    def pair_z(value, level):
        stride = 1 << level
        low = ((lane_of(value.shape) >> level) & 1) == 0
        return value + jnp.where(low, rolled(value, -stride, 1), rolled(value, stride, 1))

    barrier = pltpu.get_barrier_semaphore()
    everyone = sorted(set(BOX3 + [(i - RING if i > 8 else i, 0) for i in range(1, RING)]
                          + [(0, j - RING if j > 8 else j) for j in range(1, RING)]))
    for dx, dy in everyone:
        pl.semaphore_signal(barrier, inc=1, device_id=peer(dx, dy), device_id_type=MESH)

    total = density[0]
    for x in range(1, 16):
        total = total + density[x]
    mean_src[0] = jnp.sum(total, axis=0, keepdims=True)
    mean_x[gx] = mean_src[0]
    pl.semaphore_wait(barrier, len(everyone))

    for dx, dy in LINE_X:
        send(mean_src.at[0], mean_x.at[gx], 0, dx, dy)
    send_halo(density, 0, src, 2, 2)
    own = pl.ds(OWN[0], 16)

    def copy_own(x, j, parity):
        src[OWN[0] + x, own] = density[x]

    rows(0, 16, 16, copy_own)
    fifteen = mean_x.at[pl.ds(0, RING - 1)]
    finish(fifteen, recvs.at[0])
    row = mean_x[0]
    for i in range(1, RING):
        row = row + mean_x[i]
    mean_src[1] = row
    mean_y[gy] = row
    for dx, dy in LINE_Y:
        send(mean_src.at[1], mean_y.at[gy], 1, dx, dy)
    finish(halo_bytes, recvs.at[2])

    def coefficients(level, start, stop, step, with_target=False):
        inv = 0.25**level
        field = pot[level]
        store = co[level]

        def body(x, j, parity):
            xx, yy, zz, xy, xz, yz = hessian(field[x - 1], field[x], field[x + 1], 1 << level)
            if level:
                xx, yy, zz = xx * inv, yy * inv, zz * inv
            quarter = 0.25 * inv
            stiff_x = 1.0 + 2.0 * COUPLING * (yy + zz)
            stiff_y = 1.0 + 2.0 * COUPLING * (xx + zz)
            stiff_z = 1.0 + 2.0 * COUPLING * (xx + yy)
            diagonal = jnp.maximum(2.0 * (stiff_x + stiff_y + stiff_z), FLOOR)
            relax = (1.0 / inv) / diagonal
            if level:
                store[0, x], store[1, x], store[2, x] = stiff_x * inv, stiff_y * inv, stiff_z * inv
            else:
                store[0, x], store[1, x], store[2, x] = stiff_x, stiff_y, stiff_z
            weight = -4.0 * COUPLING * quarter * quarter
            store[3, x], store[4, x], store[5, x] = xy * weight, xz * weight, yz * weight
            store[6, x] = relax
            if with_target:
                cubic = xx * yy + xx * zz + yy * zz - (xy * xy + xz * xz + yz * yz) * 0.0625
                target = src[x] - (xx + yy + zz + 2.0 * COUPLING * cubic)
                tgt[level][x] = target
                pre[level][x] = -target * relax

        rows(start, stop, step, body)

    def jacobian(level, field, x, ys):
        parts = hessian(field[x - 1, ys], field[x, ys], field[x + 1, ys], 1 << level)
        store = co[level]
        result = store[0, x, ys] * parts[0]
        for index in range(1, 6):
            result = result + store[index, x, ys] * parts[index]
        return result

    def whole(level):
        return pl.ds(0, SIZE_Y[level])

    def first_sweep(level, start, stop, step):
        masks = red_masks(level, SIZE_Y[level], 0)
        field, store = pre[level], co[level]

        def body(x, j, parity):
            centre = field[x]
            sum_x, sum_y, sum_z, _ = neighbours(field[x - 1], centre, field[x + 1], 1 << level)
            spread = store[0, x] * sum_x + store[1, x] * sum_y + store[2, x] * sum_z
            va[level][x] = jnp.where(masks[parity], centre, centre + spread * store[6, x])

        rows(start, stop, step, body)

    def half_sweep(level, colour, start, stop, step, ys, sink=None):
        masks = red_masks(level, ys.size, ys.start)
        from_ref, to_ref = (va, vb) if colour == 0 else (vb, va)
        from_ref, to_ref = from_ref[level], to_ref[level]

        def body(x, j, parity):
            old = from_ref[x, ys]
            change = (jacobian(level, from_ref, x, ys) - tgt[level][x, ys]) * co[level][6, x, ys]
            new = jnp.where(masks[(parity + colour) % 2], old + change, old)
            if sink is None:
                to_ref[x, ys] = new
            else:
                sink(x, new)

        rows(start, stop, step, body)

    def restricted(level, start, stop, pairs, first, count, sink):
        first_x, first_y = first

        def body(x, j, parity):
            fine = first_x + 2 * x
            acc = None
            for k in range(2):
                left = tgt[level][fine + k] - jacobian(level, va[level], fine + k, whole(level))
                acc = left if acc is None else acc + left
            slot = fold.at[j]
            slot[pl.ds(0, SIZE_Y[level]), :] = pair_z(acc, level)
            sink(x, 0.125 * (slot[pl.ds(first_y, count, 2), :] + slot[pl.ds(first_y + 1, count, 2), :]))

        rows(start, stop, pairs, body)

    def averaged(level, fine, first_y, count):
        field = pot[level]
        acc = None
        for k in range(2):
            for q in range(2):
                part = field[fine + k, pl.ds(first_y + q, count, 2), :]
                acc = part if acc is None else acc + part
        return 0.125 * pair_z(acc, level)

    def prolonged(level, start, stop, step, first_y, count, coarse_of, coarse_y):
        fine_ref, coarse_ref = va[level], va[level + 1]

        def body(x, j, parity):
            value = coarse_ref[x, pl.ds(coarse_y, count)]
            for k in range(2):
                for q in range(2):
                    at = (coarse_of(x) + k, pl.ds(first_y + q, count, 2), slice(None))
                    fine_ref[at] = fine_ref[at] + value

        rows(start, stop, step, body)

    quad = lane_of((4, LANES)) & 3

    def pack(values):
        return jnp.where(
            quad == 0, values[0], jnp.where(quad == 1, values[1], jnp.where(quad == 2, values[2], values[3]))
        )

    def unpack(read, write):
        place = lane_of((28, LANES)) & 3

        def body(g, j, parity):
            value = read(g)
            turned = {d: (value if d == 0 else rolled(value, -d, 1)) for d in range(-3, 4)}
            for i in range(4):
                piece = turned[i - 3]
                for k in (2, 1, 0):
                    piece = jnp.where(place == k, turned[i - k], piece)
                write(4 * g + i, piece)

        rows(0, 2 * REACH + 1, STEP['un'], body)

    def six(field, x, ys, level):
        sum_x, sum_y, sum_z, _ = neighbours(field[x - 1, ys], field[x, ys], field[x + 1, ys], 1 << level)
        return sum_x + sum_y + sum_z

    def plain_first(level, start, stop, step):
        masks = red_masks(level, SIZE_Y[level], 0)
        relax = 4.0**level / 6.0
        field = src if level == 0 else tgt[level]

        def body(x, j, parity):
            around = six(field, x, whole(level), level)
            value = field[x]
            va[level][x] = jnp.where(masks[parity], value, value + around * (1.0 / 6.0)) * -relax

        rows(start, stop, step, body)

    def plain_restricted(level, start, stop, pairs, first, count, sink):
        first_x, first_y = first
        field = src if level == 0 else tgt[level]
        inv = 0.25**level

        def body(x, j, parity):
            fine = first_x + 2 * x
            acc = None
            for k in range(2):
                centre = va[level][fine + k]
                left = field[fine + k] - (six(va[level], fine + k, whole(level), level) - 6.0 * centre) * inv
                acc = left if acc is None else acc + left
            slot = fold.at[j]
            slot[pl.ds(0, SIZE_Y[level]), :] = pair_z(acc, level)
            sink(x, 0.125 * (slot[pl.ds(first_y, count, 2), :] + slot[pl.ds(first_y + 1, count, 2), :]))

        rows(start, stop, pairs, body)

    def plain_half(level, colour, start, stop, step, ys, sink=None):
        masks = red_masks(level, ys.size, ys.start)
        relax = 4.0**level / 6.0
        from_ref, to_ref = (va, vb) if colour == 0 else (vb, va)
        from_ref, to_ref = from_ref[level], to_ref[level]
        field = src if level == 0 else tgt[level]

        def body(x, j, parity):
            moved = six(from_ref, x, ys, level) * (1.0 / 6.0) - field[x, ys] * relax
            new = jnp.where(masks[(parity + colour) % 2], moved, from_ref[x, ys])
            if sink is None:
                to_ref[x, ys] = new
            else:
                sink(x, new)

        rows(start, stop, step, body)

    def put(ref):
        def write(x, value):
            ref[x, pl.ds(0, 28)] = value

        return write

    plain_first(0, 3, 37, STEP["b0"])

    def raw1(x, value):
        tgt1[4 + x, pl.ds(4, 16)] = value

    plain_restricted(0, 0, 16, STEP["c0"], (4, 4), 16, raw1)
    plain_first(1, 5, 19, STEP["b1"])
    raw2 = []
    plain_restricted(1, 0, 4, 4, (8, 8), 4, lambda x, value: raw2.append(value))
    packed_t[0] = pack(raw2)
    send_box(packed_t.at[0], got_0, 5)
    got_0[REACH, pl.ds(12, 4)] = packed_t[0]
    finish(fifteen, recvs.at[1])
    row = mean_y[0]
    for i in range(1, RING):
        row = row + mean_y[i]
    cells = RING * RING * 16 * 16 * LANES
    scale = 1.0 / (jnp.sum(row, axis=1, keepdims=True) * (1.0 / cells))
    finish(fifteen, sends.at[0])
    finish(fifteen, sends.at[1])
    finish(halo_bytes, sends.at[2])

    def to_source(x, j, parity):
        src[x] = src[x] * scale - 1.0

    rows(1, 39, 2, to_source)

    def to_values(level, start, stop, step):
        masks = red_masks(level, SIZE_Y[level], 0)
        relax = 4.0**level / 6.0

        def body(x, j, parity):
            va[level][x] = va[level][x] * scale + jnp.where(masks[parity], relax, 2.0 * relax)

        rows(start, stop, step, body)

    to_values(0, 10, 30, 4)
    to_values(1, 5, 19, 2)

    def to_target(x, j, parity):
        tgt1[x] = tgt1[x] * scale - 1.0

    rows(4, 20, 4, to_target)
    finish(box_u_bytes, recvs.at[5])
    unpack(lambda g: got_0[g] * scale - 1.0, put(tgt2))
    plain_first(2, 1, 27, STEP["b2"])

    def plain3(x, value):
        tgt3[1 + x] = value

    plain_restricted(2, 0, 12, STEP["c2"], (2, 0), 16, plain3)

    def way_up(half, last):
        prolonged(2, 4, 10, STEP["d2"], 8, 6, lambda x: 2 * x, 4)
        half(2, 0, 9, 19, STEP["e2"], pl.ds(8, 16))
        half(2, 1, 10, 18, STEP["f2"], pl.ds(8, 16))
        prolonged(1, 10, 18, STEP["d1"], 4, 8, lambda x: 2 * x - 16, 10)
        half(1, 0, 6, 18, STEP["e1"], whole(1))
        half(1, 1, 7, 17, STEP["f1"], whole(1))
        prolonged(0, 7, 17, STEP["d0"], 10, 10, lambda x: 2 * x - 4, 7)
        half(0, 0, 11, 29, STEP["e0"], pl.ds(8, 24))
        half(0, 1, 12, 28, STEP["f0"], pl.ds(8, 24), sink=last)

    plain_first(3, 2, 12, STEP["b3"])
    finish(box_u_bytes, sends.at[5])
    plain_half(3, 0, 3, 11, STEP["e3"], whole(3))
    plain_half(3, 1, 4, 10, STEP["f3"], whole(3))

    def set_own(x, new):
        pot0[x, own] = new[4:20]

    way_up(plain_half, set_own)

    def newton(step, carry):
        send_halo(pot0, OWN[0], pot0, 3, 4)

        def own1(x, j, parity):
            pot1[x, pl.ds(8, 8)] = averaged(0, 2 * x - 4, 12, 8)

        rows(8, 16, 8, own1)
        packed_u[...] = pack([averaged(1, 8 + 2 * x, 8, 4) for x in range(4)])
        send_box(packed_u, got_u.at[step - 1], 5 + step)
        got_u[step - 1, REACH, pl.ds(12, 4)] = packed_u[...]
        finish(side_bytes, recvs.at[3])
        coefficients(0, 13, 27, 14, with_target=True)
        finish(rest_bytes, recvs.at[4])
        coefficients(0, 2, 13, 11, with_target=True)
        coefficients(0, 27, 38, 11, with_target=True)

        def coarse1(x, j, parity):
            pot1[x, pl.ds(2, 20)] = averaged(0, 2 * x - 4, 0, 20)

        rows(3, 21, STEP["coarse1"], coarse1)
        coefficients(1, 4, 20, STEP["a1"])

        def coarse2(x, j, parity):
            pot2[x, pl.ds(10, 8)] = averaged(1, 2 * x - 16, 4, 8)

        rows(10, 18, 8, coarse2)
        coefficients(2, 12, 16, 4)
        first_sweep(0, 3, 37, STEP["b0"])

        def to_level1(x, value):
            tgt1[4 + x, pl.ds(4, 16)] = value
            pre1[4 + x, pl.ds(4, 16)] = -value * co1[6, 4 + x, pl.ds(4, 16)]

        restricted(0, 0, 16, STEP["c0"], (4, 4), 16, to_level1)
        first_sweep(1, 5, 19, STEP["b1"])
        kept = []

        def to_level2(x, value):
            kept.append((value, -value * co2[6, 12 + x, pl.ds(12, 4)]))

        restricted(1, 0, 4, 4, (8, 8), 4, to_level2)
        packed_t[0] = pack([k[0] for k in kept])
        packed_t[1] = pack([k[1] for k in kept])
        send_box(packed_t, got_t.at[step - 1], 7 + step)
        for q in range(2):
            got_t[step - 1, REACH, q, pl.ds(12, 4)] = packed_t[q]
        finish(box_u_bytes, recvs.at[5 + step])
        unpack(lambda g: got_u[step - 1, g], put(pot2))
        coefficients(2, 1, 27, STEP["a2"])

        def coarse3(x, j, parity):
            pot3[x] = averaged(2, 2 * x, 0, 16)

        rows(0, 14, STEP["coarse3"], coarse3)
        coefficients(3, 1, 13, STEP["a3"])
        finish(box_t_bytes, recvs.at[7 + step])
        unpack(lambda g: got_t[step - 1, g, 0], put(tgt2))
        unpack(lambda g: got_t[step - 1, g, 1], put(pre2))
        first_sweep(2, 1, 27, STEP["b2"])

        def to_level3(x, value):
            tgt3[1 + x] = value
            pre3[1 + x] = -value * co3[6, 1 + x]

        restricted(2, 0, 12, STEP["c2"], (2, 0), 16, to_level3)
        first_sweep(3, 2, 12, STEP["b3"])
        half_sweep(3, 0, 3, 11, STEP["e3"], whole(3))
        half_sweep(3, 1, 4, 10, STEP["f3"], whole(3))
        finish(side_bytes, sends.at[3])
        finish(rest_bytes, sends.at[4])
        finish(box_u_bytes, sends.at[5 + step])
        finish(box_t_bytes, sends.at[7 + step])

        def add_own(x, new):
            pot0[x, own] = pot0[x, own] + new[4:20]

        way_up(half_sweep, add_own)
        return carry

    lax.fori_loop(1, NEWTON, newton, 0)

    def result(x, j, parity):
        out[x] = pot0[OWN[0] + x, own]

    rows(0, 16, 16, result)


def per_device(density):
    def fields(count):
        return [
            pltpu.VMEM((SIZE_X[level], SIZE_Y[level], LANES), jnp.float32)
            for _ in range(count)
            for level in range(4)
        ]

    pots, tgts, pres, vas, vbs = (fields(1) for _ in range(5))
    cos = [pltpu.VMEM((7, SIZE_X[level], SIZE_Y[level], LANES), jnp.float32) for level in range(4)]
    return pl.pallas_call(
        kernel,
        out_shape=jax.ShapeDtypeStruct(density.shape, jnp.float32),
        in_specs=[pl.BlockSpec(memory_space=pltpu.VMEM)],
        out_specs=pl.BlockSpec(memory_space=pltpu.VMEM),
        scratch_shapes=[
            pltpu.VMEM((SIZE_X[0], SIZE_Y[0], LANES), jnp.float32),
            *pots, *tgts, *pres, *vas, *vbs, *cos,
            pltpu.VMEM((16, 40, LANES), jnp.float32),
            pltpu.VMEM((2, 4, LANES), jnp.float32),
            pltpu.VMEM((4, LANES), jnp.float32),
            pltpu.VMEM((7, 28, LANES), jnp.float32),
            pltpu.VMEM((2, 7, 2, 28, LANES), jnp.float32),
            pltpu.VMEM((2, 7, 28, LANES), jnp.float32),
            pltpu.VMEM((2, 1, LANES), jnp.float32),
            pltpu.VMEM((RING, 1, LANES), jnp.float32),
            pltpu.VMEM((RING, 1, LANES), jnp.float32),
            pltpu.SemaphoreType.DMA((10,)),
            pltpu.SemaphoreType.DMA((10,)),
        ],
        compiler_params=pltpu.CompilerParams(collective_id=0, has_side_effects=True),
    )(density)


def solution(mesh):
    return jax.shard_map(
        per_device,
        mesh=mesh,
        in_specs=(P("gx", "gy", None),),
        out_specs=P("gx", "gy", None),
        check_vma=False,
    )
```

```python
import jax
import jax.numpy as jnp
from jax import lax
from jax.experimental import pallas as pl
from jax.experimental.pallas import tpu as pltpu
from jax.sharding import PartitionSpec as P

NEWTON = 3
COUPLING = 0.1
FLOOR = 3.0
RING = 16
LANES = 128
MESH = pl.DeviceIdType.MESH

HALO = 11
OWN = (12, 8, 12, 6)
SIZE_X = (40, 24, 28, 14)
SIZE_Y = (40, 24, 32, 16)
STEP = dict(coarse1=18, a0=12, a1=8, b0=34, c0=4, b1=14, a2=26, coarse3=14, a3=12, b2=26, c2=6, b3=10, e3=8, f3=6,
            e2=10, f2=8, e1=12, f1=10, e0=18, f0=16, d2=6, d1=8, d0=10, un=7)
REACH = 3
BOX1 = [(i, j) for i in (-1, 0, 1) for j in (-1, 0, 1) if (i, j) != (0, 0)]
BOX3 = [
    (i, j)
    for i in range(-REACH, REACH + 1)
    for j in range(-REACH, REACH + 1)
    if (i, j) != (0, 0)
]
LINE_X = [(i, 0) for i in range(1, RING)]
LINE_Y = [(0, j) for j in range(1, RING)]


def rolled(value, shift, axis):
    return pltpu.roll(value, shift % value.shape[axis], axis)


def rows(start, stop, step, body):
    count = (stop - start) // step

    def block(first, offsets):
        cache = {}
        for j in offsets:
            body(first + j, j, (start + j) % 2, cache)

    if count == 1:
        block(start, range(step))
    else:
        assert step % 2 == 0 or step == 1

        def chunk(i, carry):
            block(start + i * step, range(step))
            return carry

        lax.fori_loop(0, count, chunk, 0)
    if count * step < stop - start:
        block(start, range(count * step, stop - start))


def sum_y(value):
    return rolled(value, -1, 0) + rolled(value, 1, 0)


def diff_y(value):
    return rolled(value, -1, 0) - rolled(value, 1, 0)


def sum_z(value, stride):
    return rolled(value, -stride, 1) + rolled(value, stride, 1)


def turned(ref, x, j, ys, stride, cache):
    if j not in cache:
        value = ref[x, ys]
        zp, zm = rolled(value, -stride, 1), rolled(value, stride, 1)
        cache[j] = (value, zp + zm, zp - zm)
    return cache[j]


def hessian(ref, x, j, ys, stride, cache):
    below, _, below_z = turned(ref, x - 1, j - 1, ys, stride, cache)
    centre, along_z, centre_z = turned(ref, x, j, ys, stride, cache)
    above, _, above_z = turned(ref, x + 1, j + 1, ys, stride, cache)
    twice = centre + centre
    return (
        above + below - twice,
        sum_y(centre) - twice,
        along_z - twice,
        diff_y(above - below),
        above_z - below_z,
        diff_y(centre_z),
    )


def faces(ref, x, j, ys, stride, cache, keep):
    if keep is None:
        along_z = turned(ref, x, j, ys, stride, cache)[1]
    elif j % 2 == 0:
        cache[j] = sum_z(jnp.where(keep, ref[x, ys], ref[x + 1, ys]), stride)
        along_z = cache[j]
    else:
        along_z = cache[j - 1]
    return ref[x + 1, ys] + ref[x - 1, ys], sum_y(ref[x, ys]), along_z


def kernel(
    density, out, src, pot0, pot1, pot2, pot3,
    tgt0, tgt1, tgt2, tgt3, pre0, pre1, pre2, pre3,
    va0, va1, va2, va3, vb0, vb1, vb2, vb3,
    co0, co1, co2, co3, fold, packed_t, packed_u, got_0, got_t, got_u,
    mean_src, mean_x, mean_y, sends, recvs,
):
    gx, gy = lax.axis_index("gx"), lax.axis_index("gy")
    pot = (pot0, pot1, pot2, pot3)
    tgt = (tgt0, tgt1, tgt2, tgt3)
    pre = (pre0, pre1, pre2, pre3)
    va = (va0, va1, va2, va3)
    vb = (vb0, vb1, vb2, vb3)
    co = (co0, co1, co2, co3)

    def peer(dx, dy):
        return {"gx": lax.rem(gx + dx + RING, RING), "gy": lax.rem(gy + dy + RING, RING)}

    def send(src_ref, dst_ref, which, dx, dy):
        pltpu.make_async_remote_copy(
            src_ref=src_ref,
            dst_ref=dst_ref,
            send_sem=sends.at[which],
            recv_sem=recvs.at[which],
            device_id=peer(dx, dy),
            device_id_type=MESH,
        ).start()

    def finish(ref, sem):
        pltpu.make_async_copy(ref, ref, sem).wait()

    spans = {-1: (0, HALO), 0: (0, 16), 1: (16 - HALO, HALO)}
    lands = {-1: OWN[0] + 16, 0: OWN[0], 1: OWN[0] - HALO}

    def send_halo(src_ref, src_own, dst_ref, side, rest):
        for dx, dy in [(0, 1), (0, -1)] + [o for o in BOX1 if o[0]]:
            sx, nx = spans[dx]
            sy, ny = spans[dy]
            send(
                src_ref.at[pl.ds(src_own + sx, nx), pl.ds(src_own + sy, ny)],
                dst_ref.at[pl.ds(lands[dx], nx), pl.ds(lands[dy], ny)],
                rest if dx else side, dx, dy,
            )

    halo_bytes = co0.at[0, pl.ds(0, 33), pl.ds(0, 36)]
    side_bytes = co0.at[0, pl.ds(0, 11), pl.ds(0, 32)]
    rest_bytes = co0.at[0, pl.ds(0, 38), pl.ds(0, 22)]

    def send_box(src_ref, dst_ref, which):
        for dx, dy in BOX3:
            at = pl.ds((REACH - dy) * 4, 4)
            if len(src_ref.shape) == 3:
                send(src_ref, dst_ref.at[REACH - dx, :, at], which, dx, dy)
            else:
                send(src_ref, dst_ref.at[REACH - dx, at], which, dx, dy)

    box_t_bytes = co0.at[0, pl.ds(0, 12), pl.ds(0, 32)]
    box_u_bytes = co0.at[0, pl.ds(0, 6), pl.ds(0, 32)]

    def lane_of(shape):
        return lax.broadcasted_iota(jnp.int32, shape, 1)

    def red_masks(level, size, first):
        shape = (size, LANES)
        parity = (
            lax.broadcasted_iota(jnp.int32, shape, 0) + first + (lane_of(shape) >> level)
        ) & 1
        return parity == 0, parity == 1

    def pair_z(value, level):
        stride = 1 << level
        low = ((lane_of(value.shape) >> level) & 1) == 0
        return value + jnp.where(low, rolled(value, -stride, 1), rolled(value, stride, 1))

    barrier = pltpu.get_barrier_semaphore()
    everyone = sorted(set(BOX3 + [(i - RING if i > 8 else i, 0) for i in range(1, RING)]
                          + [(0, j - RING if j > 8 else j) for j in range(1, RING)]))
    for dx, dy in everyone:
        pl.semaphore_signal(barrier, inc=1, device_id=peer(dx, dy), device_id_type=MESH)

    total = density[0]
    for x in range(1, 16):
        total = total + density[x]
    mean_src[0] = jnp.sum(total, axis=0, keepdims=True)
    mean_x[gx] = mean_src[0]
    pl.semaphore_wait(barrier, len(everyone))

    for dx, dy in LINE_X:
        send(mean_src.at[0], mean_x.at[gx], 0, dx, dy)
    send_halo(density, 0, src, 2, 2)
    own = pl.ds(OWN[0], 16)

    def copy_own(x, j, parity, cache):
        src[OWN[0] + x, own] = density[x]

    rows(0, 16, 16, copy_own)
    fifteen = mean_x.at[pl.ds(0, RING - 1)]
    finish(fifteen, recvs.at[0])
    row = mean_x[0]
    for i in range(1, RING):
        row = row + mean_x[i]
    mean_src[1] = row
    mean_y[gy] = row
    for dx, dy in LINE_Y:
        send(mean_src.at[1], mean_y.at[gy], 1, dx, dy)
    finish(halo_bytes, recvs.at[2])

    def whole(level):
        return pl.ds(0, SIZE_Y[level])

    def coefficients(level, start, stop, step, with_target=False):
        inv = 0.25**level
        field = pot[level]
        store = co[level]

        def body(x, j, parity, cache):
            xx, yy, zz, xy, xz, yz = hessian(field, x, j, whole(level), 1 << level, cache)
            if level:
                xx, yy, zz = xx * inv, yy * inv, zz * inv
            quarter = 0.25 * inv
            stiff_x = 1.0 + 2.0 * COUPLING * (yy + zz)
            stiff_y = 1.0 + 2.0 * COUPLING * (xx + zz)
            stiff_z = 1.0 + 2.0 * COUPLING * (xx + yy)
            diagonal = jnp.maximum(2.0 * (stiff_x + stiff_y + stiff_z), FLOOR)
            relax = (1.0 / inv) / diagonal
            if level:
                store[0, x], store[1, x], store[2, x] = stiff_x * inv, stiff_y * inv, stiff_z * inv
            else:
                store[0, x], store[1, x], store[2, x] = stiff_x, stiff_y, stiff_z
            weight = -4.0 * COUPLING * quarter * quarter
            store[3, x], store[4, x], store[5, x] = xy * weight, xz * weight, yz * weight
            store[6, x] = relax
            if with_target:
                cubic = xx * yy + xx * zz + yy * zz - (xy * xy + xz * xz + yz * yz) * 0.0625
                target = src[x] - (xx + yy + zz + 2.0 * COUPLING * cubic)
                tgt[level][x] = target
                pre[level][x] = -target * relax

        rows(start, stop, step, body)

    def jacobian(level, field, x, j, ys, cache):
        parts = hessian(field, x, j, ys, 1 << level, cache)
        store = co[level]
        result = store[0, x, ys] * parts[0]
        for index in range(1, 6):
            result = result + store[index, x, ys] * parts[index]
        return result

    def first_sweep(level, start, stop, step):
        masks = red_masks(level, SIZE_Y[level], 0)
        field, store = pre[level], co[level]

        def body(x, j, parity, cache):
            centre = field[x]
            along = faces(field, x, j, whole(level), 1 << level, cache, masks[parity])
            spread = store[0, x] * along[0] + store[1, x] * along[1] + store[2, x] * along[2]
            va[level][x] = jnp.where(masks[parity], centre, centre + spread * store[6, x])

        rows(start, stop, step, body)

    def half_sweep(level, colour, start, stop, step, ys, sink=None):
        masks = red_masks(level, ys.size, ys.start)
        from_ref, to_ref = (va, vb) if colour == 0 else (vb, va)
        from_ref, to_ref = from_ref[level], to_ref[level]

        def body(x, j, parity, cache):
            old = from_ref[x, ys]
            change = (jacobian(level, from_ref, x, j, ys, cache) - tgt[level][x, ys]) * co[level][6, x, ys]
            new = jnp.where(masks[(parity + colour) % 2], old + change, old)
            if sink is None:
                to_ref[x, ys] = new
            else:
                sink(x, new)

        rows(start, stop, step, body)

    def restricted(level, start, stop, pairs, first, count, sink):
        first_x, first_y = first

        def body(x, j, parity, cache):
            fine = first_x + 2 * x
            acc = None
            for k in range(2):
                left = tgt[level][fine + k] - jacobian(level, va[level], fine + k, 2 * j + k, whole(level), cache)
                acc = left if acc is None else acc + left
            slot = fold.at[j]
            slot[pl.ds(0, SIZE_Y[level]), :] = pair_z(acc, level)
            sink(x, 0.125 * (slot[pl.ds(first_y, count, 2), :] + slot[pl.ds(first_y + 1, count, 2), :]))

        rows(start, stop, pairs, body)

    def averaged(level, fine, first_y, count):
        field = pot[level]
        acc = None
        for k in range(2):
            for q in range(2):
                part = field[fine + k, pl.ds(first_y + q, count, 2), :]
                acc = part if acc is None else acc + part
        return 0.125 * pair_z(acc, level)

    def prolonged(level, start, stop, step, first_y, count, coarse_of, coarse_y):
        fine_ref, coarse_ref = va[level], va[level + 1]

        def body(x, j, parity, cache):
            value = coarse_ref[x, pl.ds(coarse_y, count)]
            for k in range(2):
                for q in range(2):
                    at = (coarse_of(x) + k, pl.ds(first_y + q, count, 2), slice(None))
                    fine_ref[at] = fine_ref[at] + value

        rows(start, stop, step, body)

    quad = lane_of((4, LANES)) & 3

    def pack(values):
        return jnp.where(
            quad == 0, values[0], jnp.where(quad == 1, values[1], jnp.where(quad == 2, values[2], values[3]))
        )

    def unpack(read, write):
        place = lane_of((28, LANES)) & 3

        def body(g, j, parity, cache):
            value = read(g)
            turned = {d: (value if d == 0 else rolled(value, -d, 1)) for d in range(-3, 4)}
            for i in range(4):
                piece = turned[i - 3]
                for k in (2, 1, 0):
                    piece = jnp.where(place == k, turned[i - k], piece)
                write(4 * g + i, piece)

        rows(0, 2 * REACH + 1, STEP['un'], body)

    def six(field, x, j, ys, level, cache, keep):
        along = faces(field, x, j, ys, 1 << level, cache, keep)
        return along[0] + along[1] + along[2]

    def plain_first(level, start, stop, step):
        masks = red_masks(level, SIZE_Y[level], 0)
        relax = 4.0**level / 6.0
        field = src if level == 0 else tgt[level]

        def body(x, j, parity, cache):
            around = six(field, x, j, whole(level), level, cache, masks[parity])
            value = field[x]
            va[level][x] = jnp.where(masks[parity], value, value + around * (1.0 / 6.0)) * -relax

        rows(start, stop, step, body)

    def plain_restricted(level, start, stop, pairs, first, count, sink):
        first_x, first_y = first
        field = src if level == 0 else tgt[level]
        inv = 0.25**level

        def body(x, j, parity, cache):
            fine = first_x + 2 * x
            acc = None
            for k in range(2):
                centre = va[level][fine + k]
                around = six(va[level], fine + k, 2 * j + k, whole(level), level, cache, None)
                left = field[fine + k] - (around - 6.0 * centre) * inv
                acc = left if acc is None else acc + left
            slot = fold.at[j]
            slot[pl.ds(0, SIZE_Y[level]), :] = pair_z(acc, level)
            sink(x, 0.125 * (slot[pl.ds(first_y, count, 2), :] + slot[pl.ds(first_y + 1, count, 2), :]))

        rows(start, stop, pairs, body)

    def plain_half(level, colour, start, stop, step, ys, sink=None):
        masks = red_masks(level, ys.size, ys.start)
        relax = 4.0**level / 6.0
        from_ref, to_ref = (va, vb) if colour == 0 else (vb, va)
        from_ref, to_ref = from_ref[level], to_ref[level]
        field = src if level == 0 else tgt[level]

        def body(x, j, parity, cache):
            other = masks[(parity + colour + 1) % 2]
            around = six(from_ref, x, j, ys, level, cache, other)
            new = jnp.where(other, from_ref[x, ys], around * (1.0 / 6.0) - field[x, ys] * relax)
            if sink is None:
                to_ref[x, ys] = new
            else:
                sink(x, new)

        rows(start, stop, step, body)

    def put(ref):
        def write(x, value):
            ref[x, pl.ds(0, 28)] = value

        return write

    plain_first(0, 3, 37, STEP["b0"])

    def raw1(x, value):
        tgt1[4 + x, pl.ds(4, 16)] = value

    plain_restricted(0, 0, 16, STEP["c0"], (4, 4), 16, raw1)
    plain_first(1, 5, 19, STEP["b1"])
    raw2 = []
    plain_restricted(1, 0, 4, 4, (8, 8), 4, lambda x, value: raw2.append(value))
    packed_t[0] = pack(raw2)
    send_box(packed_t.at[0], got_0, 5)
    got_0[REACH, pl.ds(12, 4)] = packed_t[0]
    finish(fifteen, recvs.at[1])
    row = mean_y[0]
    for i in range(1, RING):
        row = row + mean_y[i]
    cells = RING * RING * 16 * 16 * LANES
    scale = 1.0 / (jnp.sum(row, axis=1, keepdims=True) * (1.0 / cells))
    finish(fifteen, sends.at[0])
    finish(fifteen, sends.at[1])
    finish(halo_bytes, sends.at[2])

    def to_source(x, j, parity, cache):
        src[x] = src[x] * scale - 1.0

    rows(1, 39, 2, to_source)

    def to_values(level, start, stop, step):
        masks = red_masks(level, SIZE_Y[level], 0)
        relax = 4.0**level / 6.0

        def body(x, j, parity, cache):
            va[level][x] = va[level][x] * scale + jnp.where(masks[parity], relax, 2.0 * relax)

        rows(start, stop, step, body)

    to_values(0, 10, 30, 4)
    to_values(1, 5, 19, 2)

    def to_target(x, j, parity, cache):
        tgt1[x] = tgt1[x] * scale - 1.0

    rows(4, 20, 4, to_target)
    finish(box_u_bytes, recvs.at[5])
    unpack(lambda g: got_0[g] * scale - 1.0, put(tgt2))
    plain_first(2, 1, 27, STEP["b2"])

    def plain3(x, value):
        tgt3[1 + x] = value

    plain_restricted(2, 0, 12, STEP["c2"], (2, 0), 16, plain3)

    def way_up(half, last):
        prolonged(2, 4, 10, STEP["d2"], 8, 6, lambda x: 2 * x, 4)
        half(2, 0, 9, 19, STEP["e2"], pl.ds(8, 16))
        half(2, 1, 10, 18, STEP["f2"], pl.ds(8, 16))
        prolonged(1, 10, 18, STEP["d1"], 4, 8, lambda x: 2 * x - 16, 10)
        half(1, 0, 6, 18, STEP["e1"], whole(1))
        half(1, 1, 7, 17, STEP["f1"], whole(1))
        prolonged(0, 7, 17, STEP["d0"], 10, 10, lambda x: 2 * x - 4, 7)
        half(0, 0, 11, 29, STEP["e0"], pl.ds(8, 24))
        half(0, 1, 12, 28, STEP["f0"], pl.ds(8, 24), sink=last)

    plain_first(3, 2, 12, STEP["b3"])
    finish(box_u_bytes, sends.at[5])
    plain_half(3, 0, 3, 11, STEP["e3"], whole(3))
    plain_half(3, 1, 4, 10, STEP["f3"], whole(3))

    def set_own(x, new):
        pot0[x, own] = new[4:20]

    way_up(plain_half, set_own)

    def newton(step, carry):
        send_halo(pot0, OWN[0], pot0, 3, 4)

        def own1(x, j, parity, cache):
            pot1[x, pl.ds(8, 8)] = averaged(0, 2 * x - 4, 12, 8)

        rows(8, 16, 8, own1)
        packed_u[...] = pack([averaged(1, 8 + 2 * x, 8, 4) for x in range(4)])
        send_box(packed_u, got_u.at[step - 1], 5 + step)
        got_u[step - 1, REACH, pl.ds(12, 4)] = packed_u[...]
        finish(side_bytes, recvs.at[3])
        coefficients(0, 13, 27, 14, with_target=True)
        finish(rest_bytes, recvs.at[4])
        coefficients(0, 2, 13, 11, with_target=True)
        coefficients(0, 27, 38, 11, with_target=True)

        def coarse1(x, j, parity, cache):
            pot1[x, pl.ds(2, 20)] = averaged(0, 2 * x - 4, 0, 20)

        rows(3, 21, STEP["coarse1"], coarse1)
        coefficients(1, 4, 20, STEP["a1"])

        def coarse2(x, j, parity, cache):
            pot2[x, pl.ds(10, 8)] = averaged(1, 2 * x - 16, 4, 8)

        rows(10, 18, 8, coarse2)
        coefficients(2, 12, 16, 4)
        first_sweep(0, 3, 37, STEP["b0"])

        def to_level1(x, value):
            tgt1[4 + x, pl.ds(4, 16)] = value
            pre1[4 + x, pl.ds(4, 16)] = -value * co1[6, 4 + x, pl.ds(4, 16)]

        restricted(0, 0, 16, STEP["c0"], (4, 4), 16, to_level1)
        first_sweep(1, 5, 19, STEP["b1"])
        kept = []

        def to_level2(x, value):
            kept.append((value, -value * co2[6, 12 + x, pl.ds(12, 4)]))

        restricted(1, 0, 4, 4, (8, 8), 4, to_level2)
        packed_t[0] = pack([k[0] for k in kept])
        packed_t[1] = pack([k[1] for k in kept])
        send_box(packed_t, got_t.at[step - 1], 7 + step)
        for q in range(2):
            got_t[step - 1, REACH, q, pl.ds(12, 4)] = packed_t[q]
        finish(box_u_bytes, recvs.at[5 + step])
        unpack(lambda g: got_u[step - 1, g], put(pot2))
        coefficients(2, 1, 27, STEP["a2"])

        def coarse3(x, j, parity, cache):
            pot3[x] = averaged(2, 2 * x, 0, 16)

        rows(0, 14, STEP["coarse3"], coarse3)
        coefficients(3, 1, 13, STEP["a3"])
        finish(box_t_bytes, recvs.at[7 + step])
        unpack(lambda g: got_t[step - 1, g, 0], put(tgt2))
        unpack(lambda g: got_t[step - 1, g, 1], put(pre2))
        first_sweep(2, 1, 27, STEP["b2"])

        def to_level3(x, value):
            tgt3[1 + x] = value
            pre3[1 + x] = -value * co3[6, 1 + x]

        restricted(2, 0, 12, STEP["c2"], (2, 0), 16, to_level3)
        first_sweep(3, 2, 12, STEP["b3"])
        half_sweep(3, 0, 3, 11, STEP["e3"], whole(3))
        half_sweep(3, 1, 4, 10, STEP["f3"], whole(3))
        finish(side_bytes, sends.at[3])
        finish(rest_bytes, sends.at[4])
        finish(box_u_bytes, sends.at[5 + step])
        finish(box_t_bytes, sends.at[7 + step])

        def add_own(x, new):
            pot0[x, own] = pot0[x, own] + new[4:20]

        way_up(half_sweep, add_own)
        return carry

    lax.fori_loop(1, NEWTON, newton, 0)

    def result(x, j, parity, cache):
        out[x] = pot0[OWN[0] + x, own]

    rows(0, 16, 16, result)


def per_device(density):
    def fields(count):
        return [
            pltpu.VMEM((SIZE_X[level], SIZE_Y[level], LANES), jnp.float32)
            for _ in range(count)
            for level in range(4)
        ]

    pots, tgts, pres, vas, vbs = (fields(1) for _ in range(5))
    cos = [pltpu.VMEM((7, SIZE_X[level], SIZE_Y[level], LANES), jnp.float32) for level in range(4)]
    return pl.pallas_call(
        kernel,
        out_shape=jax.ShapeDtypeStruct(density.shape, jnp.float32),
        in_specs=[pl.BlockSpec(memory_space=pltpu.VMEM)],
        out_specs=pl.BlockSpec(memory_space=pltpu.VMEM),
        scratch_shapes=[
            pltpu.VMEM((SIZE_X[0], SIZE_Y[0], LANES), jnp.float32),
            *pots, *tgts, *pres, *vas, *vbs, *cos,
            pltpu.VMEM((16, 40, LANES), jnp.float32),
            pltpu.VMEM((2, 4, LANES), jnp.float32),
            pltpu.VMEM((4, LANES), jnp.float32),
            pltpu.VMEM((7, 28, LANES), jnp.float32),
            pltpu.VMEM((2, 7, 2, 28, LANES), jnp.float32),
            pltpu.VMEM((2, 7, 28, LANES), jnp.float32),
            pltpu.VMEM((2, 1, LANES), jnp.float32),
            pltpu.VMEM((RING, 1, LANES), jnp.float32),
            pltpu.VMEM((RING, 1, LANES), jnp.float32),
            pltpu.SemaphoreType.DMA((10,)),
            pltpu.SemaphoreType.DMA((10,)),
        ],
        compiler_params=pltpu.CompilerParams(collective_id=0, has_side_effects=True),
    )(density)


def solution(mesh):
    return jax.shard_map(
        per_device,
        mesh=mesh,
        in_specs=(P("gx", "gy", None),),
        out_specs=P("gx", "gy", None),
        check_vma=False,
    )
```

```python
import jax
import jax.numpy as jnp
from jax import lax
from jax.experimental import pallas as pl
from jax.experimental.pallas import tpu as pltpu
from jax.sharding import PartitionSpec as P

NEWTON = 3
COUPLING = 0.1
FLOOR = 3.0
RING = 16
LANES = 128
MESH = pl.DeviceIdType.MESH

HALO = 11
OWN = (12, 8, 12, 6)
SIZE_X = (40, 24, 28, 14)
SIZE_Y = (40, 24, 32, 16)
STEP = dict(coarse1=18, a0=12, a1=8, b0=34, c0=4, b1=14, a2=26, coarse3=14, a3=12, b2=26, c2=6, b3=10, e3=8, f3=6,
            e2=10, f2=8, e1=12, f1=10, e0=18, f0=16, d2=6, d1=8, d0=10, un=7)
REACH = 3
BOX1 = [(i, j) for i in (-1, 0, 1) for j in (-1, 0, 1) if (i, j) != (0, 0)]
BOX3 = [
    (i, j)
    for i in range(-REACH, REACH + 1)
    for j in range(-REACH, REACH + 1)
    if (i, j) != (0, 0)
]
BOX3.sort(key=lambda o: -(abs(o[0]) + 2 * abs(o[1])))
LINE_X = [(i, 0) for i in range(1, RING)]
LINE_Y = [(0, j) for j in range(1, RING)]


def rolled(value, shift, axis):
    return pltpu.roll(value, shift % value.shape[axis], axis)


def rows(start, stop, step, body):
    count = (stop - start) // step

    def block(first, offsets):
        cache = {}
        for j in offsets:
            body(first + j, j, (start + j) % 2, cache)

    if count == 1:
        block(start, range(step))
    else:
        assert step % 2 == 0 or step == 1

        def chunk(i, carry):
            block(start + i * step, range(step))
            return carry

        lax.fori_loop(0, count, chunk, 0)
    if count * step < stop - start:
        block(start, range(count * step, stop - start))


def sum_y(value):
    return rolled(value, -1, 0) + rolled(value, 1, 0)


def diff_y(value):
    return rolled(value, -1, 0) - rolled(value, 1, 0)


def sum_z(value, stride):
    return rolled(value, -stride, 1) + rolled(value, stride, 1)


def turned(ref, x, j, ys, stride, cache):
    if j not in cache:
        value = ref[x, ys]
        zp, zm = rolled(value, -stride, 1), rolled(value, stride, 1)
        cache[j] = (value, zp + zm, zp - zm)
    return cache[j]


def hessian(ref, x, j, ys, stride, cache):
    below, _, below_z = turned(ref, x - 1, j - 1, ys, stride, cache)
    centre, along_z, centre_z = turned(ref, x, j, ys, stride, cache)
    above, _, above_z = turned(ref, x + 1, j + 1, ys, stride, cache)
    twice = centre + centre
    return (
        above + below - twice,
        sum_y(centre) - twice,
        along_z - twice,
        diff_y(above - below),
        above_z - below_z,
        diff_y(centre_z),
    )


def faces(ref, x, j, ys, stride, cache, keep):
    if keep is None:
        along_z = turned(ref, x, j, ys, stride, cache)[1]
    elif j % 2 == 0:
        cache[j] = sum_z(jnp.where(keep, ref[x, ys], ref[x + 1, ys]), stride)
        along_z = cache[j]
    else:
        along_z = cache[j - 1]
    return ref[x + 1, ys] + ref[x - 1, ys], sum_y(ref[x, ys]), along_z


def kernel(
    density, out, src, pot0, pot1, pot2, pot3,
    tgt0, tgt1, tgt2, tgt3, pre0, pre1, pre2, pre3,
    va0, va1, va2, va3, vb0, vb1, vb2, vb3,
    co0, co1, co2, co3, fold, packed_t, packed_u, got_0, got_t, got_u,
    mean_src, mean_x, mean_y, sends, recvs, local,
):
    gx, gy = lax.axis_index("gx"), lax.axis_index("gy")
    pot = (pot0, pot1, pot2, pot3)
    tgt = (tgt0, tgt1, tgt2, tgt3)
    pre = (pre0, pre1, pre2, pre3)
    va = (va0, va1, va2, va3)
    vb = (vb0, vb1, vb2, vb3)
    co = (co0, co1, co2, co3)

    def peer(dx, dy):
        return {"gx": lax.rem(gx + dx + RING, RING), "gy": lax.rem(gy + dy + RING, RING)}

    def send(src_ref, dst_ref, which, dx, dy):
        pltpu.make_async_remote_copy(
            src_ref=src_ref,
            dst_ref=dst_ref,
            send_sem=sends.at[which],
            recv_sem=recvs.at[which],
            device_id=peer(dx, dy),
            device_id_type=MESH,
        ).start()

    def finish(ref, sem):
        pltpu.make_async_copy(ref, ref, sem).wait()

    def send_halo(ref, width, side, rest):
        spans = {-1: (0, width), 0: (0, 16), 1: (16 - width, width)}
        lands = {-1: OWN[0] + 16, 0: OWN[0], 1: OWN[0] - width}
        for dx, dy in [(0, 1), (0, -1)] + [o for o in BOX1 if o[0] and o[1]] + [(1, 0), (-1, 0)]:
            sx, nx = spans[dx]
            sy, ny = spans[dy]
            send(
                ref.at[pl.ds(OWN[0] + sx, nx), pl.ds(OWN[0] + sy, ny)],
                ref.at[pl.ds(lands[dx], nx), pl.ds(lands[dy], ny)],
                rest if dx else side, dx, dy,
            )

    halo_bytes = co0.at[0, pl.ds(0, 26), pl.ds(0, 40)]
    side_bytes = co0.at[0, pl.ds(0, 11), pl.ds(0, 32)]
    rest_bytes = co0.at[0, pl.ds(0, 38), pl.ds(0, 22)]

    def send_box(src_ref, dst_ref, which):
        for dx, dy in BOX3:
            at = pl.ds((REACH - dy) * 4, 4)
            if len(src_ref.shape) == 3:
                send(src_ref, dst_ref.at[REACH - dx, :, at], which, dx, dy)
            else:
                send(src_ref, dst_ref.at[REACH - dx, at], which, dx, dy)

    box_t_bytes = co0.at[0, pl.ds(0, 12), pl.ds(0, 32)]
    box_u_bytes = co0.at[0, pl.ds(0, 6), pl.ds(0, 32)]

    def lane_of(shape):
        return lax.broadcasted_iota(jnp.int32, shape, 1)

    def red_masks(level, size, first):
        shape = (size, LANES)
        parity = (
            lax.broadcasted_iota(jnp.int32, shape, 0) + first + (lane_of(shape) >> level)
        ) & 1
        return parity == 0, parity == 1

    def pair_z(value, level):
        stride = 1 << level
        low = ((lane_of(value.shape) >> level) & 1) == 0
        return value + jnp.where(low, rolled(value, -stride, 1), rolled(value, stride, 1))

    fetch = pltpu.make_async_copy(density, src.at[pl.ds(OWN[0], 16), pl.ds(OWN[0], 16)], local.at[0])
    fetch.start()
    barrier = pltpu.get_barrier_semaphore()
    everyone = sorted(set(BOX3 + [(i - RING if i > 8 else i, 0) for i in range(1, RING)]
                          + [(0, j - RING if j > 8 else j) for j in range(1, RING)]))
    for dx, dy in everyone:
        pl.semaphore_signal(barrier, inc=1, device_id=peer(dx, dy), device_id_type=MESH)

    own = pl.ds(OWN[0], 16)
    fetch.wait()
    total = src[OWN[0], own]
    for x in range(1, 16):
        total = total + src[OWN[0] + x, own]
    mean_src[0] = jnp.sum(total, axis=0, keepdims=True)
    mean_x[gx] = mean_src[0]
    pl.semaphore_wait(barrier, len(everyone))

    send_halo(src, HALO - 1, 2, 2)
    for dx, dy in LINE_X:
        send(mean_src.at[0], mean_x.at[gx], 0, dx, dy)
    fifteen = mean_x.at[pl.ds(0, RING - 1)]
    finish(fifteen, recvs.at[0])
    row = mean_x[0]
    for i in range(1, RING):
        row = row + mean_x[i]
    mean_src[1] = row
    mean_y[gy] = row
    for dx, dy in LINE_Y:
        send(mean_src.at[1], mean_y.at[gy], 1, dx, dy)
    finish(halo_bytes, recvs.at[2])

    def whole(level):
        return pl.ds(0, SIZE_Y[level])

    def coefficients(level, start, stop, step, with_target=False):
        inv = 0.25**level
        field = pot[level]
        store = co[level]

        def body(x, j, parity, cache):
            xx, yy, zz, xy, xz, yz = hessian(field, x, j, whole(level), 1 << level, cache)
            if level:
                xx, yy, zz = xx * inv, yy * inv, zz * inv
            quarter = 0.25 * inv
            stiff_x = 1.0 + 2.0 * COUPLING * (yy + zz)
            stiff_y = 1.0 + 2.0 * COUPLING * (xx + zz)
            stiff_z = 1.0 + 2.0 * COUPLING * (xx + yy)
            diagonal = jnp.maximum(2.0 * (stiff_x + stiff_y + stiff_z), FLOOR)
            relax = (1.0 / inv) / diagonal
            if level:
                store[0, x], store[1, x], store[2, x] = stiff_x * inv, stiff_y * inv, stiff_z * inv
            else:
                store[0, x], store[1, x], store[2, x] = stiff_x, stiff_y, stiff_z
            weight = -4.0 * COUPLING * quarter * quarter
            store[3, x], store[4, x], store[5, x] = xy * weight, xz * weight, yz * weight
            store[6, x] = relax
            if with_target:
                cubic = xx * yy + xx * zz + yy * zz - (xy * xy + xz * xz + yz * yz) * 0.0625
                target = src[x] - (xx + yy + zz + 2.0 * COUPLING * cubic)
                tgt[level][x] = target
                pre[level][x] = -target * relax

        rows(start, stop, step, body)

    def jacobian(level, field, x, j, ys, cache):
        parts = hessian(field, x, j, ys, 1 << level, cache)
        store = co[level]
        result = store[0, x, ys] * parts[0]
        for index in range(1, 6):
            result = result + store[index, x, ys] * parts[index]
        return result

    def first_sweep(level, start, stop, step):
        masks = red_masks(level, SIZE_Y[level], 0)
        field, store = pre[level], co[level]

        def body(x, j, parity, cache):
            centre = field[x]
            along = faces(field, x, j, whole(level), 1 << level, cache, masks[parity])
            spread = store[0, x] * along[0] + store[1, x] * along[1] + store[2, x] * along[2]
            va[level][x] = jnp.where(masks[parity], centre, centre + spread * store[6, x])

        rows(start, stop, step, body)

    def half_sweep(level, colour, start, stop, step, ys, sink=None):
        masks = red_masks(level, ys.size, ys.start)
        from_ref, to_ref = (va, vb) if colour == 0 else (vb, va)
        from_ref, to_ref = from_ref[level], to_ref[level]

        def body(x, j, parity, cache):
            old = from_ref[x, ys]
            change = (jacobian(level, from_ref, x, j, ys, cache) - tgt[level][x, ys]) * co[level][6, x, ys]
            new = jnp.where(masks[(parity + colour) % 2], old + change, old)
            if sink is None:
                to_ref[x, ys] = new
            else:
                sink(x, new)

        rows(start, stop, step, body)

    def restricted(level, start, stop, pairs, first, count, sink):
        first_x, first_y = first

        def body(x, j, parity, cache):
            fine = first_x + 2 * x
            acc = None
            for k in range(2):
                left = tgt[level][fine + k] - jacobian(level, va[level], fine + k, 2 * j + k, whole(level), cache)
                acc = left if acc is None else acc + left
            slot = fold.at[j]
            slot[pl.ds(0, SIZE_Y[level]), :] = pair_z(acc, level)
            sink(x, 0.125 * (slot[pl.ds(first_y, count, 2), :] + slot[pl.ds(first_y + 1, count, 2), :]))

        rows(start, stop, pairs, body)

    def averaged(level, fine, first_y, count):
        field = pot[level]
        acc = None
        for k in range(2):
            for q in range(2):
                part = field[fine + k, pl.ds(first_y + q, count, 2), :]
                acc = part if acc is None else acc + part
        return 0.125 * pair_z(acc, level)

    def prolonged(level, start, stop, step, first_y, count, coarse_of, coarse_y):
        fine_ref, coarse_ref = va[level], va[level + 1]

        def body(x, j, parity, cache):
            value = coarse_ref[x, pl.ds(coarse_y, count)]
            for k in range(2):
                for q in range(2):
                    at = (coarse_of(x) + k, pl.ds(first_y + q, count, 2), slice(None))
                    fine_ref[at] = fine_ref[at] + value

        rows(start, stop, step, body)

    quad = lane_of((4, LANES)) & 3

    def pack(values):
        return jnp.where(
            quad == 0, values[0], jnp.where(quad == 1, values[1], jnp.where(quad == 2, values[2], values[3]))
        )

    def unpack(read, write):
        place = lane_of((28, LANES)) & 3

        def body(g, j, parity, cache):
            value = read(g)
            turned = {d: (value if d == 0 else rolled(value, -d, 1)) for d in range(-3, 4)}
            for i in range(4):
                piece = turned[i - 3]
                for k in (2, 1, 0):
                    piece = jnp.where(place == k, turned[i - k], piece)
                write(4 * g + i, piece)

        rows(0, 2 * REACH + 1, STEP['un'], body)

    def six(field, x, j, ys, level, cache, keep):
        along = faces(field, x, j, ys, 1 << level, cache, keep)
        return along[0] + along[1] + along[2]

    def plain_first(level, start, stop, step):
        masks = red_masks(level, SIZE_Y[level], 0)
        relax = 4.0**level / 6.0
        field = src if level == 0 else tgt[level]

        def body(x, j, parity, cache):
            around = six(field, x, j, whole(level), level, cache, masks[parity])
            value = field[x]
            va[level][x] = jnp.where(masks[parity], value, value + around * (1.0 / 6.0)) * -relax

        rows(start, stop, step, body)

    def plain_restricted(level, start, stop, pairs, first, count, sink):
        first_x, first_y = first
        field = src if level == 0 else tgt[level]
        inv = 0.25**level

        def body(x, j, parity, cache):
            fine = first_x + 2 * x
            acc = None
            for k in range(2):
                centre = va[level][fine + k]
                around = six(va[level], fine + k, 2 * j + k, whole(level), level, cache, None)
                left = field[fine + k] - (around - 6.0 * centre) * inv
                acc = left if acc is None else acc + left
            slot = fold.at[j]
            slot[pl.ds(0, SIZE_Y[level]), :] = pair_z(acc, level)
            sink(x, 0.125 * (slot[pl.ds(first_y, count, 2), :] + slot[pl.ds(first_y + 1, count, 2), :]))

        rows(start, stop, pairs, body)

    def plain_half(level, colour, start, stop, step, ys, sink=None):
        masks = red_masks(level, ys.size, ys.start)
        relax = 4.0**level / 6.0
        from_ref, to_ref = (va, vb) if colour == 0 else (vb, va)
        from_ref, to_ref = from_ref[level], to_ref[level]
        field = src if level == 0 else tgt[level]

        def body(x, j, parity, cache):
            other = masks[(parity + colour + 1) % 2]
            around = six(from_ref, x, j, ys, level, cache, other)
            new = jnp.where(other, from_ref[x, ys], around * (1.0 / 6.0) - field[x, ys] * relax)
            if sink is None:
                to_ref[x, ys] = new
            else:
                sink(x, new)

        rows(start, stop, step, body)

    def put(ref):
        def write(x, value):
            ref[x, pl.ds(0, 28)] = value

        return write

    plain_first(0, 3, 37, STEP["b0"])

    def raw1(x, value):
        tgt1[4 + x, pl.ds(4, 16)] = value

    plain_restricted(0, 0, 16, STEP["c0"], (4, 4), 16, raw1)
    plain_first(1, 5, 19, STEP["b1"])
    raw2 = []
    plain_restricted(1, 0, 4, 4, (8, 8), 4, lambda x, value: raw2.append(value))
    packed_t[0] = pack(raw2)
    send_box(packed_t.at[0], got_0, 5)
    got_0[REACH, pl.ds(12, 4)] = packed_t[0]
    finish(fifteen, recvs.at[1])
    row = mean_y[0]
    for i in range(1, RING):
        row = row + mean_y[i]
    cells = RING * RING * 16 * 16 * LANES
    scale = 1.0 / (jnp.sum(row, axis=1, keepdims=True) * (1.0 / cells))
    finish(fifteen, sends.at[0])
    finish(fifteen, sends.at[1])
    finish(halo_bytes, sends.at[2])

    def to_source(x, j, parity, cache):
        src[x] = src[x] * scale - 1.0

    rows(1, 39, 2, to_source)

    def to_values(level, start, stop, step):
        masks = red_masks(level, SIZE_Y[level], 0)
        relax = 4.0**level / 6.0

        def body(x, j, parity, cache):
            va[level][x] = va[level][x] * scale + jnp.where(masks[parity], relax, 2.0 * relax)

        rows(start, stop, step, body)

    to_values(0, 10, 30, 4)
    to_values(1, 5, 19, 2)

    def to_target(x, j, parity, cache):
        tgt1[x] = tgt1[x] * scale - 1.0

    rows(4, 20, 4, to_target)
    finish(box_u_bytes, recvs.at[5])
    unpack(lambda g: got_0[g] * scale - 1.0, put(tgt2))
    plain_first(2, 1, 27, STEP["b2"])

    def plain3(x, value):
        tgt3[1 + x] = value

    plain_restricted(2, 0, 12, STEP["c2"], (2, 0), 16, plain3)

    def way_up(half, last):
        prolonged(2, 4, 10, STEP["d2"], 8, 6, lambda x: 2 * x, 4)
        half(2, 0, 9, 19, STEP["e2"], pl.ds(8, 16))
        half(2, 1, 10, 18, STEP["f2"], pl.ds(8, 16))
        prolonged(1, 10, 18, STEP["d1"], 4, 8, lambda x: 2 * x - 16, 10)
        half(1, 0, 6, 18, STEP["e1"], whole(1))
        half(1, 1, 7, 17, STEP["f1"], whole(1))
        prolonged(0, 7, 17, STEP["d0"], 10, 10, lambda x: 2 * x - 4, 7)
        half(0, 0, 11, 29, STEP["e0"], pl.ds(8, 24))
        half(0, 1, 12, 28, STEP["f0"], pl.ds(8, 24), sink=last)

    plain_first(3, 2, 12, STEP["b3"])
    finish(box_u_bytes, sends.at[5])
    plain_half(3, 0, 3, 11, STEP["e3"], whole(3))
    plain_half(3, 1, 4, 10, STEP["f3"], whole(3))

    def set_own(x, new):
        pot0[x, own] = new[4:20]

    way_up(plain_half, set_own)

    def newton(step, carry):
        send_halo(pot0, HALO, 3, 4)

        def own1(x, j, parity, cache):
            pot1[x, pl.ds(8, 8)] = averaged(0, 2 * x - 4, 12, 8)

        rows(8, 16, 8, own1)
        packed_u[...] = pack([averaged(1, 8 + 2 * x, 8, 4) for x in range(4)])
        send_box(packed_u, got_u.at[step - 1], 5 + step)
        got_u[step - 1, REACH, pl.ds(12, 4)] = packed_u[...]
        finish(side_bytes, recvs.at[3])
        coefficients(0, 13, 27, 14, with_target=True)
        finish(rest_bytes, recvs.at[4])
        coefficients(0, 2, 13, 11, with_target=True)
        coefficients(0, 27, 38, 11, with_target=True)

        def coarse1(x, j, parity, cache):
            pot1[x, pl.ds(2, 20)] = averaged(0, 2 * x - 4, 0, 20)

        rows(3, 21, STEP["coarse1"], coarse1)
        coefficients(1, 4, 20, STEP["a1"])

        def coarse2(x, j, parity, cache):
            pot2[x, pl.ds(10, 8)] = averaged(1, 2 * x - 16, 4, 8)

        rows(10, 18, 8, coarse2)
        coefficients(2, 12, 16, 4)
        first_sweep(0, 3, 37, STEP["b0"])

        def to_level1(x, value):
            tgt1[4 + x, pl.ds(4, 16)] = value
            pre1[4 + x, pl.ds(4, 16)] = -value * co1[6, 4 + x, pl.ds(4, 16)]

        restricted(0, 0, 16, STEP["c0"], (4, 4), 16, to_level1)
        first_sweep(1, 5, 19, STEP["b1"])
        kept = []

        def to_level2(x, value):
            kept.append((value, -value * co2[6, 12 + x, pl.ds(12, 4)]))

        restricted(1, 0, 4, 4, (8, 8), 4, to_level2)
        packed_t[0] = pack([k[0] for k in kept])
        packed_t[1] = pack([k[1] for k in kept])
        send_box(packed_t, got_t.at[step - 1], 7 + step)
        for q in range(2):
            got_t[step - 1, REACH, q, pl.ds(12, 4)] = packed_t[q]
        finish(box_u_bytes, recvs.at[5 + step])
        unpack(lambda g: got_u[step - 1, g], put(pot2))
        coefficients(2, 1, 27, STEP["a2"])

        def coarse3(x, j, parity, cache):
            pot3[x] = averaged(2, 2 * x, 0, 16)

        rows(0, 14, STEP["coarse3"], coarse3)
        coefficients(3, 1, 13, STEP["a3"])
        finish(box_t_bytes, recvs.at[7 + step])
        unpack(lambda g: got_t[step - 1, g, 0], put(tgt2))
        unpack(lambda g: got_t[step - 1, g, 1], put(pre2))
        first_sweep(2, 1, 27, STEP["b2"])

        def to_level3(x, value):
            tgt3[1 + x] = value
            pre3[1 + x] = -value * co3[6, 1 + x]

        restricted(2, 0, 12, STEP["c2"], (2, 0), 16, to_level3)
        first_sweep(3, 2, 12, STEP["b3"])
        half_sweep(3, 0, 3, 11, STEP["e3"], whole(3))
        half_sweep(3, 1, 4, 10, STEP["f3"], whole(3))
        finish(side_bytes, sends.at[3])
        finish(rest_bytes, sends.at[4])
        finish(box_u_bytes, sends.at[5 + step])
        finish(box_t_bytes, sends.at[7 + step])

        def add_own(x, new):
            pot0[x, own] = pot0[x, own] + new[4:20]

        way_up(half_sweep, add_own)
        return carry

    lax.fori_loop(1, NEWTON, newton, 0)

    def result(x, j, parity, cache):
        out[x] = pot0[OWN[0] + x, own]

    rows(0, 16, 16, result)


def per_device(density):
    def fields(count):
        return [
            pltpu.VMEM((SIZE_X[level], SIZE_Y[level], LANES), jnp.float32)
            for _ in range(count)
            for level in range(4)
        ]

    pots, tgts, pres, vas, vbs = (fields(1) for _ in range(5))
    cos = [pltpu.VMEM((7, SIZE_X[level], SIZE_Y[level], LANES), jnp.float32) for level in range(4)]
    return pl.pallas_call(
        kernel,
        out_shape=jax.ShapeDtypeStruct(density.shape, jnp.float32),
        in_specs=[pl.BlockSpec(memory_space=pltpu.HBM)],
        out_specs=pl.BlockSpec(memory_space=pltpu.VMEM),
        scratch_shapes=[
            pltpu.VMEM((SIZE_X[0], SIZE_Y[0], LANES), jnp.float32),
            *pots, *tgts, *pres, *vas, *vbs, *cos,
            pltpu.VMEM((16, 40, LANES), jnp.float32),
            pltpu.VMEM((2, 4, LANES), jnp.float32),
            pltpu.VMEM((4, LANES), jnp.float32),
            pltpu.VMEM((7, 28, LANES), jnp.float32),
            pltpu.VMEM((2, 7, 2, 28, LANES), jnp.float32),
            pltpu.VMEM((2, 7, 28, LANES), jnp.float32),
            pltpu.VMEM((2, 1, LANES), jnp.float32),
            pltpu.VMEM((RING, 1, LANES), jnp.float32),
            pltpu.VMEM((RING, 1, LANES), jnp.float32),
            pltpu.SemaphoreType.DMA((10,)),
            pltpu.SemaphoreType.DMA((10,)),
            pltpu.SemaphoreType.DMA((1,)),
        ],
        compiler_params=pltpu.CompilerParams(collective_id=0, has_side_effects=True, vmem_limit_bytes=32 << 20),
    )(density)


def solution(mesh):
    return jax.shard_map(
        per_device,
        mesh=mesh,
        in_specs=(P("gx", "gy", None),),
        out_specs=P("gx", "gy", None),
        check_vma=False,
    )
```

```python
import jax
import jax.numpy as jnp
from jax import lax
from jax.experimental import pallas as pl
from jax.experimental.pallas import tpu as pltpu
from jax.sharding import PartitionSpec as P

NEWTON = 3
COUPLING = 0.1
FLOOR = 3.0
RING = 16
LANES = 128
MESH = pl.DeviceIdType.MESH

HALO = 11
OWN = (12, 8, 12, 6)
SIZE_X = (40, 24, 28, 14)
SIZE_Y = (40, 24, 32, 16)
STEP = dict(coarse1=18, a0=12, a1=8, b0=34, c0=4, b1=14, a2=26, coarse3=14, a3=12, b2=26, c2=6, b3=10, e3=8, f3=6,
            e2=10, f2=8, e1=12, f1=10, e0=18, f0=16, d2=6, d1=8, d0=10, un=7)
REACH = 3
BOX1 = [(i, j) for i in (-1, 0, 1) for j in (-1, 0, 1) if (i, j) != (0, 0)]
BOX3 = [
    (i, j)
    for i in range(-REACH, REACH + 1)
    for j in range(-REACH, REACH + 1)
    if (i, j) != (0, 0)
]
BOX3.sort(key=lambda o: -(abs(o[0]) + 2 * abs(o[1])))
LINE_X = [(i, 0) for i in range(1, RING)]
LINE_Y = [(0, j) for j in range(1, RING)]


def rolled(value, shift, axis):
    return pltpu.roll(value, shift % value.shape[axis], axis)


def rows(start, stop, step, body):
    count = (stop - start) // step

    def block(first, offsets):
        cache = {}
        for j in offsets:
            body(first + j, j, (start + j) % 2, cache)

    if count == 1:
        block(start, range(step))
    else:
        assert step % 2 == 0 or step == 1

        def chunk(i, carry):
            block(start + i * step, range(step))
            return carry

        lax.fori_loop(0, count, chunk, 0)
    if count * step < stop - start:
        block(start, range(count * step, stop - start))


def sum_y(value):
    return rolled(value, -1, 0) + rolled(value, 1, 0)


def diff_y(value):
    return rolled(value, -1, 0) - rolled(value, 1, 0)


def sum_z(value, stride):
    return rolled(value, -stride, 1) + rolled(value, stride, 1)


def turned(ref, x, j, ys, stride, cache):
    if j not in cache:
        value = ref[x, ys]
        zp, zm = rolled(value, -stride, 1), rolled(value, stride, 1)
        cache[j] = (value, zp + zm, zp - zm)
    return cache[j]


def hessian(ref, x, j, ys, stride, cache):
    below, _, below_z = turned(ref, x - 1, j - 1, ys, stride, cache)
    centre, along_z, centre_z = turned(ref, x, j, ys, stride, cache)
    above, _, above_z = turned(ref, x + 1, j + 1, ys, stride, cache)
    twice = centre + centre
    return (
        above + below - twice,
        sum_y(centre) - twice,
        along_z - twice,
        diff_y(above - below),
        above_z - below_z,
        diff_y(centre_z),
    )


def faces(ref, x, j, ys, stride, cache, keep):
    if keep is None:
        along_z = turned(ref, x, j, ys, stride, cache)[1]
    elif j % 2 == 0:
        cache[j] = sum_z(jnp.where(keep, ref[x, ys], ref[x + 1, ys]), stride)
        along_z = cache[j]
    else:
        along_z = cache[j - 1]
    return ref[x + 1, ys] + ref[x - 1, ys], sum_y(ref[x, ys]), along_z


def kernel(
    density, out, src, pot0, pot1, pot2, pot3,
    tgt0, tgt1, tgt2, tgt3, pre0, pre1, pre2, pre3,
    va0, va1, va2, va3, vb0, vb1, vb2, vb3,
    co0, co1, co2, co3, fold, packed_t, packed_u, got_0, got_t, got_u,
    mean_src, mean_x, mean_y, sends, recvs, local,
):
    gx, gy = lax.axis_index("gx"), lax.axis_index("gy")
    pot = (pot0, pot1, pot2, pot3)
    tgt = (tgt0, tgt1, tgt2, tgt3)
    pre = (pre0, pre1, pre2, pre3)
    va = (va0, va1, va2, va3)
    vb = (vb0, vb1, vb2, vb3)
    co = (co0, co1, co2, co3)

    def peer(dx, dy):
        return {"gx": lax.rem(gx + dx + RING, RING), "gy": lax.rem(gy + dy + RING, RING)}

    def send(src_ref, dst_ref, which, dx, dy):
        pltpu.make_async_remote_copy(
            src_ref=src_ref,
            dst_ref=dst_ref,
            send_sem=sends.at[which],
            recv_sem=recvs.at[which],
            device_id=peer(dx, dy),
            device_id_type=MESH,
        ).start()

    def finish(ref, sem):
        pltpu.make_async_copy(ref, ref, sem).wait()

    def send_halo(ref, width, side, rest):
        spans = {-1: (0, width), 0: (0, 16), 1: (16 - width, width)}
        lands = {-1: OWN[0] + 16, 0: OWN[0], 1: OWN[0] - width}
        for dx, dy in [(0, 1), (0, -1)] + [o for o in BOX1 if o[0] and o[1]] + [(1, 0), (-1, 0)]:
            sx, nx = spans[dx]
            sy, ny = spans[dy]
            send(
                ref.at[pl.ds(OWN[0] + sx, nx), pl.ds(OWN[0] + sy, ny)],
                ref.at[pl.ds(lands[dx], nx), pl.ds(lands[dy], ny)],
                rest if dx else side, dx, dy,
            )

    halo_bytes = co0.at[0, pl.ds(0, 26), pl.ds(0, 40)]
    side_bytes = co0.at[0, pl.ds(0, 11), pl.ds(0, 32)]
    rest_bytes = co0.at[0, pl.ds(0, 38), pl.ds(0, 22)]

    def send_box(src_ref, dst_ref, which):
        for dx, dy in BOX3:
            at = pl.ds((REACH - dy) * 4, 4)
            if len(src_ref.shape) == 3:
                send(src_ref, dst_ref.at[REACH - dx, :, at], which, dx, dy)
            else:
                send(src_ref, dst_ref.at[REACH - dx, at], which, dx, dy)

    box_t_bytes = co0.at[0, pl.ds(0, 12), pl.ds(0, 32)]
    box_u_bytes = co0.at[0, pl.ds(0, 6), pl.ds(0, 32)]

    def lane_of(shape):
        return lax.broadcasted_iota(jnp.int32, shape, 1)

    def red_masks(level, size, first):
        shape = (size, LANES)
        parity = (
            lax.broadcasted_iota(jnp.int32, shape, 0) + first + (lane_of(shape) >> level)
        ) & 1
        return parity == 0, parity == 1

    def pair_z(value, level):
        stride = 1 << level
        low = ((lane_of(value.shape) >> level) & 1) == 0
        return value + jnp.where(low, rolled(value, -stride, 1), rolled(value, stride, 1))

    fetch = pltpu.make_async_copy(density, src.at[pl.ds(OWN[0], 16), pl.ds(OWN[0], 16)], local.at[0])
    fetch.start()
    barrier = pltpu.get_barrier_semaphore()
    everyone = sorted(set(BOX3 + [(i - RING if i > 8 else i, 0) for i in range(1, RING)]
                          + [(0, j - RING if j > 8 else j) for j in range(1, RING)]))
    for dx, dy in everyone:
        pl.semaphore_signal(barrier, inc=1, device_id=peer(dx, dy), device_id_type=MESH)

    own = pl.ds(OWN[0], 16)
    fetch.wait()
    total = src[OWN[0], own]
    for x in range(1, 16):
        total = total + src[OWN[0] + x, own]
    mean_src[0] = jnp.sum(total, axis=0, keepdims=True)
    mean_x[gx] = mean_src[0]
    pl.semaphore_wait(barrier, len(everyone))

    send_halo(src, HALO - 1, 2, 2)
    for dx, dy in LINE_X:
        send(mean_src.at[0], mean_x.at[gx], 0, dx, dy)
    fifteen = mean_x.at[pl.ds(0, RING - 1)]
    finish(fifteen, recvs.at[0])
    row = mean_x[0]
    for i in range(1, RING):
        row = row + mean_x[i]
    mean_src[1] = row
    mean_y[gy] = row
    for dx, dy in LINE_Y:
        send(mean_src.at[1], mean_y.at[gy], 1, dx, dy)
    finish(halo_bytes, recvs.at[2])

    def whole(level):
        return pl.ds(0, SIZE_Y[level])

    def coefficients(level, start, stop, step, with_target=False):
        inv = 0.25**level
        field = pot[level]
        store = co[level]

        def body(x, j, parity, cache):
            xx, yy, zz, xy, xz, yz = hessian(field, x, j, whole(level), 1 << level, cache)
            if level:
                xx, yy, zz = xx * inv, yy * inv, zz * inv
            quarter = 0.25 * inv
            stiff_x = 1.0 + 2.0 * COUPLING * (yy + zz)
            stiff_y = 1.0 + 2.0 * COUPLING * (xx + zz)
            stiff_z = 1.0 + 2.0 * COUPLING * (xx + yy)
            diagonal = jnp.maximum(2.0 * (stiff_x + stiff_y + stiff_z), FLOOR)
            relax = (1.0 / inv) / diagonal
            if level:
                store[0, x], store[1, x], store[2, x] = stiff_x * inv, stiff_y * inv, stiff_z * inv
            else:
                store[0, x], store[1, x], store[2, x] = stiff_x, stiff_y, stiff_z
            weight = -4.0 * COUPLING * quarter * quarter
            store[3, x], store[4, x], store[5, x] = xy * weight, xz * weight, yz * weight
            store[6, x] = relax
            if with_target:
                cubic = xx * yy + xx * zz + yy * zz - (xy * xy + xz * xz + yz * yz) * 0.0625
                target = src[x] - (xx + yy + zz + 2.0 * COUPLING * cubic)
                tgt[level][x] = target
                pre[level][x] = -target * relax

        rows(start, stop, step, body)

    def jacobian(level, field, x, j, ys, cache):
        parts = hessian(field, x, j, ys, 1 << level, cache)
        store = co[level]
        result = store[0, x, ys] * parts[0]
        for index in range(1, 6):
            result = result + store[index, x, ys] * parts[index]
        return result

    def first_sweep(level, start, stop, step):
        masks = red_masks(level, SIZE_Y[level], 0)
        field, store = pre[level], co[level]

        def body(x, j, parity, cache):
            centre = field[x]
            along = faces(field, x, j, whole(level), 1 << level, cache, masks[parity])
            spread = store[0, x] * along[0] + store[1, x] * along[1] + store[2, x] * along[2]
            va[level][x] = jnp.where(masks[parity], centre, centre + spread * store[6, x])

        rows(start, stop, step, body)

    def half_sweep(level, colour, start, stop, step, ys, sink=None):
        masks = red_masks(level, ys.size, ys.start)
        from_ref, to_ref = (va, vb) if colour == 0 else (vb, va)
        from_ref, to_ref = from_ref[level], to_ref[level]

        def body(x, j, parity, cache):
            old = from_ref[x, ys]
            change = (jacobian(level, from_ref, x, j, ys, cache) - tgt[level][x, ys]) * co[level][6, x, ys]
            new = jnp.where(masks[(parity + colour) % 2], old + change, old)
            if sink is None:
                to_ref[x, ys] = new
            else:
                sink(x, new)

        rows(start, stop, step, body)

    def restricted(level, start, stop, pairs, first, count, sink):
        first_x, first_y = first

        def body(x, j, parity, cache):
            fine = first_x + 2 * x
            acc = None
            for k in range(2):
                left = tgt[level][fine + k] - jacobian(level, va[level], fine + k, 2 * j + k, whole(level), cache)
                acc = left if acc is None else acc + left
            slot = fold.at[j]
            slot[pl.ds(0, SIZE_Y[level]), :] = pair_z(acc, level)
            sink(x, 0.125 * (slot[pl.ds(first_y, count, 2), :] + slot[pl.ds(first_y + 1, count, 2), :]))

        rows(start, stop, pairs, body)

    def averaged(level, fine, first_y, count):
        field = pot[level]
        acc = None
        for k in range(2):
            for q in range(2):
                part = field[fine + k, pl.ds(first_y + q, count, 2), :]
                acc = part if acc is None else acc + part
        return 0.125 * pair_z(acc, level)

    def prolonged(level, start, stop, step, first_y, count, coarse_of, coarse_y):
        fine_ref, coarse_ref = va[level], va[level + 1]

        def body(x, j, parity, cache):
            value = coarse_ref[x, pl.ds(coarse_y, count)]
            for k in range(2):
                for q in range(2):
                    at = (coarse_of(x) + k, pl.ds(first_y + q, count, 2), slice(None))
                    fine_ref[at] = fine_ref[at] + value

        rows(start, stop, step, body)

    quad = lane_of((4, LANES)) & 3

    def pack(values):
        return jnp.where(
            quad == 0, values[0], jnp.where(quad == 1, values[1], jnp.where(quad == 2, values[2], values[3]))
        )

    def unpack(read, write):
        place = lane_of((28, LANES)) & 3

        def body(g, j, parity, cache):
            value = read(g)
            turned = {d: (value if d == 0 else rolled(value, -d, 1)) for d in range(-3, 4)}
            for i in range(4):
                piece = turned[i - 3]
                for k in (2, 1, 0):
                    piece = jnp.where(place == k, turned[i - k], piece)
                write(4 * g + i, piece)

        rows(0, 2 * REACH + 1, STEP['un'], body)

    def six(field, x, j, ys, level, cache, keep):
        along = faces(field, x, j, ys, 1 << level, cache, keep)
        return along[0] + along[1] + along[2]

    def plain_first(level, start, stop, step):
        masks = red_masks(level, SIZE_Y[level], 0)
        relax = 4.0**level / 6.0
        field = src if level == 0 else tgt[level]

        def body(x, j, parity, cache):
            around = six(field, x, j, whole(level), level, cache, masks[parity])
            value = field[x]
            va[level][x] = jnp.where(masks[parity], value, value + around * (1.0 / 6.0)) * -relax

        rows(start, stop, step, body)

    def plain_restricted(level, start, stop, pairs, first, count, sink):
        first_x, first_y = first
        field = src if level == 0 else tgt[level]
        inv = 0.25**level

        def body(x, j, parity, cache):
            fine = first_x + 2 * x
            acc = None
            for k in range(2):
                centre = va[level][fine + k]
                around = six(va[level], fine + k, 2 * j + k, whole(level), level, cache, None)
                left = field[fine + k] - (around - 6.0 * centre) * inv
                acc = left if acc is None else acc + left
            slot = fold.at[j]
            slot[pl.ds(0, SIZE_Y[level]), :] = pair_z(acc, level)
            sink(x, 0.125 * (slot[pl.ds(first_y, count, 2), :] + slot[pl.ds(first_y + 1, count, 2), :]))

        rows(start, stop, pairs, body)

    def plain_half(level, colour, start, stop, step, ys, sink=None):
        masks = red_masks(level, ys.size, ys.start)
        relax = 4.0**level / 6.0
        from_ref, to_ref = (va, vb) if colour == 0 else (vb, va)
        from_ref, to_ref = from_ref[level], to_ref[level]
        field = src if level == 0 else tgt[level]

        def body(x, j, parity, cache):
            other = masks[(parity + colour + 1) % 2]
            around = six(from_ref, x, j, ys, level, cache, other)
            new = jnp.where(other, from_ref[x, ys], around * (1.0 / 6.0) - field[x, ys] * relax)
            if sink is None:
                to_ref[x, ys] = new
            else:
                sink(x, new)

        rows(start, stop, step, body)

    def put(ref):
        def write(x, value):
            ref[x, pl.ds(0, 28)] = value

        return write

    plain_first(0, 3, 37, STEP["b0"])

    def raw1(x, value):
        tgt1[4 + x, pl.ds(4, 16)] = value

    plain_restricted(0, 0, 16, STEP["c0"], (4, 4), 16, raw1)
    plain_first(1, 5, 19, STEP["b1"])
    raw2 = []
    plain_restricted(1, 0, 4, 4, (8, 8), 4, lambda x, value: raw2.append(value))
    packed_t[0] = pack(raw2)
    send_box(packed_t.at[0], got_0, 5)
    got_0[REACH, pl.ds(12, 4)] = packed_t[0]
    finish(fifteen, recvs.at[1])
    row = mean_y[0]
    for i in range(1, RING):
        row = row + mean_y[i]
    cells = RING * RING * 16 * 16 * LANES
    scale = 1.0 / (jnp.sum(row, axis=1, keepdims=True) * (1.0 / cells))
    finish(fifteen, sends.at[0])
    finish(fifteen, sends.at[1])
    finish(halo_bytes, sends.at[2])

    def to_source(x, j, parity, cache):
        src[x] = src[x] * scale - 1.0

    rows(1, 39, 2, to_source)

    def to_values(level, start, stop, step):
        masks = red_masks(level, SIZE_Y[level], 0)
        relax = 4.0**level / 6.0

        def body(x, j, parity, cache):
            va[level][x] = va[level][x] * scale + jnp.where(masks[parity], relax, 2.0 * relax)

        rows(start, stop, step, body)

    to_values(0, 10, 30, 4)
    to_values(1, 5, 19, 2)

    def to_target(x, j, parity, cache):
        tgt1[x] = tgt1[x] * scale - 1.0

    rows(4, 20, 4, to_target)
    finish(box_u_bytes, recvs.at[5])
    unpack(lambda g: got_0[g] * scale - 1.0, put(tgt2))
    plain_first(2, 1, 27, STEP["b2"])

    def plain3(x, value):
        tgt3[1 + x] = value

    plain_restricted(2, 0, 12, STEP["c2"], (2, 0), 16, plain3)

    def way_up(half, last):
        prolonged(2, 4, 10, STEP["d2"], 8, 6, lambda x: 2 * x, 4)
        half(2, 0, 9, 19, STEP["e2"], pl.ds(8, 16))
        half(2, 1, 10, 18, STEP["f2"], pl.ds(8, 16))
        prolonged(1, 10, 18, STEP["d1"], 4, 8, lambda x: 2 * x - 16, 10)
        half(1, 0, 6, 18, STEP["e1"], whole(1))
        half(1, 1, 7, 17, STEP["f1"], whole(1))
        prolonged(0, 7, 17, STEP["d0"], 10, 10, lambda x: 2 * x - 4, 7)
        half(0, 0, 11, 29, STEP["e0"], pl.ds(8, 24))
        half(0, 1, 12, 28, STEP["f0"], pl.ds(8, 24), sink=last)

    plain_first(3, 2, 12, STEP["b3"])
    finish(box_u_bytes, sends.at[5])
    plain_half(3, 0, 3, 11, STEP["e3"], whole(3))
    plain_half(3, 1, 4, 10, STEP["f3"], whole(3))

    def set_own(x, new):
        pot0[x, own] = new[4:20]

    way_up(plain_half, set_own)

    def newton(step, carry):
        send_halo(pot0, HALO, 3, 4)

        finish(side_bytes, recvs.at[3])
        coefficients(0, 13, 27, 14, with_target=True)
        finish(rest_bytes, recvs.at[4])

        def coarse1(x, j, parity, cache):
            pot1[x, pl.ds(2, 20)] = averaged(0, 2 * x - 4, 0, 20)

        rows(3, 21, STEP["coarse1"], coarse1)
        packed_u[...] = pack([averaged(1, 8 + 2 * x, 8, 4) for x in range(4)])
        send_box(packed_u, got_u.at[step - 1], 5 + step)
        got_u[step - 1, REACH, pl.ds(12, 4)] = packed_u[...]
        coefficients(0, 2, 13, 11, with_target=True)
        coefficients(0, 27, 38, 11, with_target=True)

        coefficients(1, 4, 20, STEP["a1"])

        def coarse2(x, j, parity, cache):
            pot2[x, pl.ds(10, 8)] = averaged(1, 2 * x - 16, 4, 8)

        rows(10, 18, 8, coarse2)
        coefficients(2, 12, 16, 4)
        first_sweep(0, 3, 37, STEP["b0"])

        def to_level1(x, value):
            tgt1[4 + x, pl.ds(4, 16)] = value
            pre1[4 + x, pl.ds(4, 16)] = -value * co1[6, 4 + x, pl.ds(4, 16)]

        restricted(0, 0, 16, STEP["c0"], (4, 4), 16, to_level1)
        first_sweep(1, 5, 19, STEP["b1"])
        kept = []

        def to_level2(x, value):
            kept.append((value, -value * co2[6, 12 + x, pl.ds(12, 4)]))

        restricted(1, 0, 4, 4, (8, 8), 4, to_level2)
        packed_t[0] = pack([k[0] for k in kept])
        packed_t[1] = pack([k[1] for k in kept])
        send_box(packed_t, got_t.at[step - 1], 7 + step)
        for q in range(2):
            got_t[step - 1, REACH, q, pl.ds(12, 4)] = packed_t[q]
        finish(box_u_bytes, recvs.at[5 + step])
        unpack(lambda g: got_u[step - 1, g], put(pot2))
        coefficients(2, 1, 27, STEP["a2"])

        def coarse3(x, j, parity, cache):
            pot3[x] = averaged(2, 2 * x, 0, 16)

        rows(0, 14, STEP["coarse3"], coarse3)
        coefficients(3, 1, 13, STEP["a3"])
        finish(box_t_bytes, recvs.at[7 + step])
        unpack(lambda g: got_t[step - 1, g, 0], put(tgt2))
        unpack(lambda g: got_t[step - 1, g, 1], put(pre2))
        first_sweep(2, 1, 27, STEP["b2"])

        def to_level3(x, value):
            tgt3[1 + x] = value
            pre3[1 + x] = -value * co3[6, 1 + x]

        restricted(2, 0, 12, STEP["c2"], (2, 0), 16, to_level3)
        first_sweep(3, 2, 12, STEP["b3"])
        half_sweep(3, 0, 3, 11, STEP["e3"], whole(3))
        half_sweep(3, 1, 4, 10, STEP["f3"], whole(3))
        finish(side_bytes, sends.at[3])
        finish(rest_bytes, sends.at[4])
        finish(box_u_bytes, sends.at[5 + step])
        finish(box_t_bytes, sends.at[7 + step])

        def add_own(x, new):
            pot0[x, own] = pot0[x, own] + new[4:20]

        way_up(half_sweep, add_own)
        return carry

    lax.fori_loop(1, NEWTON, newton, 0)

    def result(x, j, parity, cache):
        out[x] = pot0[OWN[0] + x, own]

    rows(0, 16, 16, result)


def per_device(density):
    def fields(count):
        return [
            pltpu.VMEM((SIZE_X[level], SIZE_Y[level], LANES), jnp.float32)
            for _ in range(count)
            for level in range(4)
        ]

    pots, tgts, pres, vas, vbs = (fields(1) for _ in range(5))
    cos = [pltpu.VMEM((7, SIZE_X[level], SIZE_Y[level], LANES), jnp.float32) for level in range(4)]
    return pl.pallas_call(
        kernel,
        out_shape=jax.ShapeDtypeStruct(density.shape, jnp.float32),
        in_specs=[pl.BlockSpec(memory_space=pltpu.HBM)],
        out_specs=pl.BlockSpec(memory_space=pltpu.VMEM),
        scratch_shapes=[
            pltpu.VMEM((SIZE_X[0], SIZE_Y[0], LANES), jnp.float32),
            *pots, *tgts, *pres, *vas, *vbs, *cos,
            pltpu.VMEM((16, 40, LANES), jnp.float32),
            pltpu.VMEM((2, 4, LANES), jnp.float32),
            pltpu.VMEM((4, LANES), jnp.float32),
            pltpu.VMEM((7, 28, LANES), jnp.float32),
            pltpu.VMEM((2, 7, 2, 28, LANES), jnp.float32),
            pltpu.VMEM((2, 7, 28, LANES), jnp.float32),
            pltpu.VMEM((2, 1, LANES), jnp.float32),
            pltpu.VMEM((RING, 1, LANES), jnp.float32),
            pltpu.VMEM((RING, 1, LANES), jnp.float32),
            pltpu.SemaphoreType.DMA((10,)),
            pltpu.SemaphoreType.DMA((10,)),
            pltpu.SemaphoreType.DMA((1,)),
        ],
        compiler_params=pltpu.CompilerParams(collective_id=0, has_side_effects=True, vmem_limit_bytes=32 << 20),
    )(density)


def solution(mesh):
    return jax.shard_map(
        per_device,
        mesh=mesh,
        in_specs=(P("gx", "gy", None),),
        out_specs=P("gx", "gy", None),
        check_vma=False,
    )
```
